512 devices in a mesh: leaf: 128 (over z, x, core), lvl: 4 (over y).
Axes of the slice: x: 4, y: 4, z: 16, core: 2. Of those that a mesh axis runs over, the one named last changes fastest.
Arguments:
- offsets: float32 [3, 262144], P(None, 'leaf'), may hold values from -0.5 to 0.5
- vel_cot: float32 [3, 262144], P(None, 'leaf'), may hold values from -0.18 to 0.18
- m2l_ops: bfloat16 [16, 456, 456], P('lvl'), may hold values from -0.25 to 0.25
- child_ops: bfloat16 [8, 456, 456], P('lvl'), may hold values from -0.25 to 0.25
- check_map: float32 [456, 456], replicated, may hold values from -0.015625 to 0.015625
- leaf_dest: int32 [4, 4096, 4, 1], P('lvl', 'leaf'), may hold values from 0 to 127; in each aligned block of 128 rows (0 to 127, 128 to 255, ..., all dimensions but the last counted through in order) at most 2 rows name the same one
- leaf_slot: int32 [4, 4096, 4], P('lvl', 'leaf'), may hold values from 0 to 31
- coarse_dest: int32 [4, 512, 4, 1], P('lvl'), may hold values from 0 to 127
- coarse_slot: int32 [4, 512, 4], P('lvl'), may hold values from 0 to 3
- near_box: int32 [4096, 16], P('leaf', 'lvl'), may hold values from 0 to 31
- near_dir: int32 [4096, 16], P('leaf', 'lvl'), may hold values from 0 to 26
Outputs:
- force_cot: float32 [3, 262144], P(None, 'leaf')
The draws below stay inside these ranges and needn't reach their ends.
Inputs may be any that keep to these rules, and one draw needn't show every extreme that they name: `leaf_dest`: in the rows of one device (aligned blocks of 128 rows in the order of the leading dimensions) no subtree is named more than 2 times. `near_box`: A place among the 32 leaf boxes of the same subtree.
All inputs are finite; a program needn't handle non-finite values.
Results may differ from the reference program's by a relative error of at most 0.0095.
Values may be sent and summed in bfloat16 or wider, within the bound.
A program may use at most 64 MiB of HBM per device.

```python
import math
import jax
import jax.numpy as jnp
import numpy as np
from jax import lax

SIDE = 6
M = 456
CLASSES = 16
NEAR = 16
LB_DEV = 32
PPB = 64
LEAF = 4096
PARENT = 512
CB_DEV = 4
PARTICLES = 262144
CL_DEV = 4
ITEMS = 128
CAP = 2
N_LEAF = 128
N_LVL = 4


def with_ends(entries, rng, least, high):
    shape = entries.shape
    spot = [jax.random.randint(jax.random.fold_in(rng, axis), (), 0, shape[axis]) for axis in range(len(shape))]
    entries = entries.at[tuple(spot)].set(least)
    longest = shape.index(max(shape))
    spot[longest] = (spot[longest] + 1) % shape[longest]
    return entries.at[tuple(spot)].set(high)


def level_of(own_key, extent, pieces, smallest, high):
    gain, own = 1.0, jax.random.fold_in(own_key, 6)
    for position, shards_of in pieces:
        heights = jnp.exp(jax.random.uniform(jax.random.fold_in(own, position), (shards_of,), jnp.float32, smallest / len(pieces), high / len(pieces)))
        gain = gain * jnp.repeat(heights, extent[position] // shards_of).reshape([-1 if axis == position else 1 for axis in range(len(extent))])
    return gain


def assign_block(key, own, number, rows, count, top, bound, skew):
    sequence = jax.random.permutation(key, count)
    crowded, ordinary = shares(count, rows * top, bound, skew, True), shares(count, rows * top, bound, skew, False)
    places = jnp.arange(count)

    def named(tallies, offset_by):
        used = int((tallies > 0).sum())
        fixed = max(1, used // 4)
        moved = fixed + (places - fixed + offset_by * (used - fixed)) % max(1, count - fixed)
        return jnp.zeros((count,), jnp.int32).at[sequence[jnp.where(places < fixed, places, moved)]].set(jnp.asarray(tallies, jnp.int32))

    tallies = jnp.where(number % 4 == 0, named(crowded, number // 4), named(ordinary, number - number // 4 - 1))
    mixed = jax.random.permutation(jax.random.fold_in(own, 3), count)
    donor, taker = mixed[0:count // 2 * 2:2], mixed[1:count // 2 * 2:2]
    room = jnp.minimum(tallies[donor] - 1, bound - tallies[taker]) // 2
    room = jnp.where((donor == sequence[0]) | (taker == sequence[0]) | (tallies[taker] == 0), 0, jnp.maximum(room, 0))
    moved = jax.random.randint(jax.random.fold_in(own, 4), (count // 2,), 0, 1 << 20) % (room + 1)
    tallies = tallies.at[donor].add(-moved).at[taker].add(moved)
    members = jnp.searchsorted(jnp.cumsum(tallies), jnp.arange(rows * top), side="right").astype(jnp.int32)
    table = members.reshape(top, rows).T
    table = table[jax.random.permutation(jax.random.fold_in(own, 1), rows)]
    offset_by = jax.random.randint(jax.random.fold_in(own, 2), (rows, 1), 0, top)
    return jnp.take_along_axis(table, (jnp.arange(top)[None, :] + offset_by) % top, axis=1)


def shares(number_of, total, bound, lean, full):
    weights = [(1 << 20) // math.isqrt(standing ** lean) + 1 for standing in range(1, number_of + 1)]
    largest = bound if full else min(bound, max(-(-total // number_of), total * weights[0] // sum(weights)))
    least = 1 if total - largest >= number_of - 1 else 0
    holding, surplus = [largest] + [least] * (number_of - 1), total - largest - least * (number_of - 1)
    while surplus > 0:
        movable = [i for i in range(1, number_of) if holding[i] < largest] or [i for i in range(1, number_of) if holding[i] < bound]
        whole, remaining = sum([weights[i] for i in movable]), surplus
        for i in movable:
            more = min(bound - holding[i], max(1, remaining * weights[i] // whole), surplus)
            holding[i] = holding[i] + more
            surplus = surplus - more
    return np.array(holding)


def centred(rng, shape, deviation, bound, cuts=(), held_as=jnp.bfloat16):
    drawn = jax.random.normal(rng, shape, jnp.float32) * deviation
    if len(cuts) > 0:
        drawn = level_of(rng, shape, cuts, -0.22, 0.18) * drawn
    return jnp.clip(drawn, min=-bound, max=bound).astype(held_as)


def setup_inputs(seed: int = 0) -> dict:
    key_list = jax.random.split(jax.random.key(seed), 12)
    offsets = jnp.clip(jax.random.uniform(key_list[0], (3, PARTICLES), jnp.float32, -0.5, 0.5) * level_of(key_list[0], (3, PARTICLES), ((1, 128),), -0.4, 0.0), -0.5, 0.5)
    vel_cot = centred(key_list[1], (3, PARTICLES), 0.03, 0.18, ((1, 128),), jnp.float32)
    m2l_ops = centred(key_list[2], (CLASSES, M, M), M ** -0.5, 0.25, ((0, 4),))
    child_ops = centred(key_list[3], (8, M, M), M ** -0.5, 0.25, ((0, 4),))
    check_map = centred(key_list[4], (M, M), (M * 256) ** -0.5, 0.015625, (), jnp.float32)
    leaf_dest_keys = jax.random.split(jax.random.fold_in(key_list[5], 1), N_LVL * LEAF * CL_DEV // ITEMS)
    leaf_dest_turns = jax.random.permutation(jax.random.fold_in(key_list[5], 3), N_LVL * LEAF * CL_DEV // ITEMS)
    leaf_dest = jax.vmap(lambda own, number: assign_block(jax.random.fold_in(key_list[5], 2), own, number, ITEMS, N_LEAF, 1, CAP, 2))(leaf_dest_keys, leaf_dest_turns).reshape((N_LVL, LEAF, CL_DEV, 1))
    leaf_slot = with_ends(jax.random.randint(key_list[6], (N_LVL, LEAF, CL_DEV), 0, LB_DEV), jax.random.fold_in(key_list[6], 1), 0, LB_DEV - 1).astype(jnp.int32)
    coarse_dest = with_ends(jax.random.randint(key_list[7], (N_LVL, PARENT, CL_DEV, 1), 0, N_LEAF), jax.random.fold_in(key_list[7], 1), 0, N_LEAF - 1).astype(jnp.int32)
    coarse_slot = with_ends(jax.random.randint(key_list[8], (N_LVL, PARENT, CL_DEV), 0, CB_DEV), jax.random.fold_in(key_list[8], 1), 0, CB_DEV - 1).astype(jnp.int32)
    near_box = with_ends(jax.random.randint(key_list[9], (LEAF, NEAR), 0, LB_DEV), jax.random.fold_in(key_list[9], 1), 0, LB_DEV - 1).astype(jnp.int32)
    near_dir = with_ends(jax.random.randint(key_list[10], (LEAF, NEAR), 0, 27), jax.random.fold_in(key_list[10], 1), 0, 26).astype(jnp.int32)
    return {"offsets": offsets, "vel_cot": vel_cot, "m2l_ops": m2l_ops, "child_ops": child_ops, "check_map": check_map, "leaf_dest": leaf_dest, "leaf_slot": leaf_slot, "coarse_dest": coarse_dest, "coarse_slot": coarse_slot, "near_box": near_box, "near_dir": near_dir}


EPSILON2 = 0.01
RADIUS = 0.525


def surface_points(edge_count):
    levels = np.linspace(-1.0, 1.0, edge_count)
    lattice = np.stack(np.meshgrid(levels, levels, levels, indexing="ij"), 0).reshape(3, -1)
    on_shell = np.max(np.abs(lattice), 0) > 1.0 - 1e-9
    return jnp.asarray(lattice[:, on_shell] * RADIUS, jnp.float32)


def stokes_apply(relative, source):
    squared = jnp.sum(relative * relative, axis=0)
    weights = (squared + EPSILON2) ** -1.5
    spread = source[..., None, :]
    along = jnp.sum(relative * spread, axis=0)
    return jnp.sum(weights * ((squared + 2.0 * EPSILON2) * spread + relative * along), axis=-1)


def to_surface(points, vectors, shell):
    relative = shell[:, None, :, None] - points[:, :, None, :]
    values = stokes_apply(relative, vectors)
    return values.transpose(1, 0, 2).reshape(values.shape[1], -1)


def from_surface(points, density, shell):
    source = density.reshape(density.shape[0], 3, -1).transpose(1, 0, 2)
    relative = points[:, :, :, None] - shell[:, None, None, :]
    return stokes_apply(relative, source)


def directions(codes):
    return jnp.stack([codes // 9 - 1, codes // 3 % 3 - 1, codes % 3 - 1], 0).astype(jnp.float32)


def near_terms(points, src_points, src_vectors, shifts):
    moved = src_points + shifts[..., None]
    relative = points[:, :, None, :, None] - moved[:, :, :, None, :]
    return jnp.sum(stokes_apply(relative, src_vectors), axis=2)


def reference(offsets, vel_cot, m2l_ops, child_ops, check_map, leaf_dest, leaf_slot, coarse_dest, coarse_slot, near_box, near_dir):
    shell = surface_points(SIDE)
    points = offsets.reshape(3, LEAF, PPB)
    vectors = vel_cot.reshape(3, LEAF, PPB)
    blocks = LEAF // 8
    point_blocks = points.reshape(3, blocks, 8, PPB).transpose(1, 0, 2, 3)
    vector_blocks = vectors.reshape(3, blocks, 8, PPB).transpose(1, 0, 2, 3)
    local_float = lax.map(lambda packed: to_surface(packed[0], packed[1], shell), (point_blocks, vector_blocks))
    leaf_local = local_float.reshape(LEAF, M).astype(jnp.bfloat16)

    owners = leaf_dest[..., 0].transpose(0, 2, 1).reshape(CLASSES, LEAF)
    places = leaf_slot.transpose(0, 2, 1).reshape(CLASSES, LEAF)
    sources = (owners * LB_DEV + places).astype(jnp.int32)

    def leaf_class(total, packed):
        operator, targets = packed
        term = jnp.dot(leaf_local, operator, preferred_element_type=jnp.float32).astype(jnp.bfloat16)
        return total + jax.ops.segment_sum(term.astype(jnp.float32), targets, num_segments=LEAF), None

    leaf_mult, _ = lax.scan(leaf_class, jnp.zeros((LEAF, M), jnp.float32), (m2l_ops, sources))

    children = leaf_local.reshape(PARENT, 8, M)
    parent_float = jnp.zeros((PARENT, M), jnp.float32)
    for octant in range(8):
        parent_float = parent_float + jnp.dot(children[:, octant], child_ops[octant], preferred_element_type=jnp.float32)
    parent_local = parent_float.astype(jnp.bfloat16)

    coarse_global = coarse_dest[..., 0] * CB_DEV + coarse_slot
    coarse_ids = coarse_global.transpose(0, 2, 1).reshape(CLASSES, PARENT).astype(jnp.int32)

    def coarse_class(total, packed):
        operator, targets = packed
        term = 0.5 * jnp.dot(parent_local, operator, preferred_element_type=jnp.float32)
        return total + jax.ops.segment_sum(term, targets, num_segments=PARENT), None

    parent_float, _ = lax.scan(coarse_class, jnp.zeros((PARENT, M), jnp.float32), (m2l_ops, coarse_ids))
    parent_mult = parent_float.astype(jnp.bfloat16)
    lowered = jnp.stack([jnp.dot(parent_mult, child_ops[octant].T, preferred_element_type=jnp.float32) for octant in range(8)], 1)
    total_mult = leaf_mult + lowered.reshape(LEAF, M)
    check_cot = jnp.dot(total_mult, check_map, precision=lax.Precision.HIGHEST)

    check_blocks = check_cot.reshape(blocks, 8, M)
    far_blocks = lax.map(lambda packed: from_surface(packed[0], packed[1], shell), (point_blocks, check_blocks))
    far_cot = far_blocks.transpose(1, 0, 2, 3).reshape(3, PARTICLES)

    bases = (jnp.arange(LEAF, dtype=jnp.int32) // LB_DEV) * LB_DEV
    neighbours = (bases[:, None] + near_box).astype(jnp.int32)
    shifts = directions(near_dir)
    neighbour_blocks = neighbours.reshape(blocks, 8, NEAR)
    shift_blocks = shifts.reshape(3, blocks, 8, NEAR).transpose(1, 0, 2, 3)

    def near_block(packed):
        here, chosen, moved = packed
        return near_terms(here, points[:, chosen], vectors[:, chosen], moved)

    near_blocks = lax.map(near_block, (point_blocks, neighbour_blocks, shift_blocks))
    near_cot = near_blocks.transpose(1, 0, 2, 3).reshape(3, PARTICLES)
    return far_cot + near_cot
```

```python
import jax
import jax.numpy as jnp
import numpy as np
from jax import lax
from jax.experimental import pallas as pl
from jax.experimental.pallas import tpu as pltpu
from jax.sharding import PartitionSpec as P

SIDE = 6
EPS = 0.01
RADIUS = 0.525
M = 456
K = 152
NZ, NX, NL = 16, 8, 4
CH = 120
F32, BF16 = jnp.float32, jnp.bfloat16
MESH = pl.DeviceIdType.MESH


def surface_points():
    levels = np.linspace(-1.0, 1.0, SIDE)
    lattice = np.stack(np.meshgrid(levels, levels, levels, indexing="ij"), 0).reshape(3, -1)
    on_shell = np.max(np.abs(lattice), 0) > 1.0 - 1e-09
    return (lattice[:, on_shell] * RADIUS).astype(np.float32)


def iota(shape, dim):
    return lax.broadcasted_iota(jnp.int32, shape, dim)


def dot(a, b, dims=((1,), (0,))):
    return lax.dot_general(a, b, (dims, ((), ())), preferred_element_type=F32)


def one_hot(hits):
    return jnp.where(hits, 1.0, 0.0).astype(BF16)


def kernel(
    off, vel, m2l_h, child_h, cm_h, ids_ref, meta, shell, near_box, near_dir,
    out_ref,
    m2l, child, cm, cmt, x6, nat, tn, tab, xg, wst, qst, av, ppb, prs, idr, gz, pall, spb, spr,
    cpb, cpr, tms, sb, rb, fin, wt, fl, nn, fo, frb, frr,
    loc, ss, rs,
):
    me, lv = lax.axis_index("leaf"), lax.axis_index("lvl")
    zi, xi = me // NX, lax.rem(me, NX)

    def z_peer(k):
        return lax.rem(zi + k, NZ)

    def x_peer(k):
        return lax.rem(xi + k, NX)

    def y_peer(k):
        return lax.rem(lv + k, NL)

    barrier = pltpu.get_barrier_semaphore()

    def greet_z(k, c):
        pl.semaphore_signal(barrier, 1, device_id=(z_peer(k) * NX + xi, lv), device_id_type=MESH)
        return c

    def greet_x(k, c):
        pl.semaphore_signal(barrier, 1, device_id=(zi * NX + x_peer(k), lv), device_id_type=MESH)
        return c

    def greet_y(k, c):
        pl.semaphore_signal(barrier, 1, device_id=(me, y_peer(k)), device_id_type=MESH)
        return c

    lax.fori_loop(1, NZ, greet_z, 0)
    lax.fori_loop(1, NX, greet_x, 0)
    lax.fori_loop(1, NL, greet_y, 0)

    load_child = pltpu.make_async_copy(child_h, child, loc.at[0])
    load_m2l = pltpu.make_async_copy(m2l_h, m2l, loc.at[1])
    load_cm = pltpu.make_async_copy(cm_h, cm, loc.at[2])
    load_child.start()
    load_m2l.start()
    load_cm.start()

    def send(src, dst, phase, device):
        pltpu.make_async_remote_copy(
            src_ref=src, dst_ref=dst, send_sem=ss.at[phase], recv_sem=rs.at[phase],
            device_id=device, device_id_type=MESH,
        ).start()

    def arrived(ref, phase):
        pltpu.make_async_copy(ref, ref, rs.at[phase]).wait()

    def gone(ref, phase):
        pltpu.make_async_copy(ref, ref, ss.at[phase]).wait()

    x6[0:3] = off[...]
    x6[3:6] = vel[...]
    x6[6:8] = jnp.zeros((2, 2048), F32)
    low = iota((8, 128), 1) < 64
    for m in range(16):
        v = x6[:, m * 128 : (m + 1) * 128]
        nat[pl.ds(m, 8, stride=16), :] = v
        r = pltpu.roll(v, 64, 1)
        tab[2 * m] = jnp.where(low, v, r)
        tab[2 * m + 1] = jnp.where(low, r, v)
    tn[...] = nat[...].T
    lane16 = iota((16, 128), 1) // 16
    for c in range(6):
        total = jnp.zeros((16, 128), F32)
        for b2 in range(2):
            for g in range(4):
                j, pos = b2 * 4 + g, g * 2 + b2
                piece = pltpu.roll(tn[16 * j : 16 * j + 16, :], (16 * (pos - c)) % 128, 1)
                total = jnp.where(lane16 == pos, piece, total)
        xg[c] = total

    def to_surface(kb, carry):
        row = pl.multiple_of(kb * 8, 8)
        s = [shell[pl.ds(c * K + row, 8), :] for c in range(3)]
        acc = [jnp.zeros((8, 128), F32) for _ in range(3)]
        for i in range(16):
            r = [s[c] - xg[c, i : i + 1, :] for c in range(3)]
            v = [xg[3 + c, i : i + 1, :] for c in range(3)]
            t = r[0] * r[0] + r[1] * r[1] + r[2] * r[2] + EPS
            inv = lax.rsqrt(t)
            w = inv * inv * inv
            q = w * (t + EPS)
            wd = w * (r[0] * v[0] + r[1] * v[1] + r[2] * v[2])
            for c in range(3):
                acc[c] = acc[c] + (q * v[c] + wd * r[c])
            wst[i, pl.ds(row, 8), :] = w
            qst[i, pl.ds(row, 8), :] = q
        for c in range(3):
            av[pl.ds(c * K + row, 8), :] = acc[c]
        return carry

    lax.fori_loop(0, K // 8, to_surface, 0)
    a = av[...]
    a = a + pltpu.roll(a, 64, 1)
    a = a + pltpu.roll(a, 32, 1)
    b_row, b_lane = iota((32, 128), 0), iota((32, 128), 1)
    pick = one_hot(b_lane == lax.rem(b_row, 2) * 16 + b_row // 2)
    local = dot(pick, a.astype(BF16), ((1,), (1,))).astype(BF16)

    p_row, c_col = iota((8, 32), 0), iota((8, 32), 1)
    load_child.wait()
    part = jnp.zeros((8, M), F32)
    for o in range(2):
        rows = one_hot((c_col == p_row * 8 + lv * 2 + o) & (p_row < 4))
        part = part + dot(dot(rows, local).astype(BF16), child[o])
    ppb[3] = jnp.zeros((8, 128), F32)
    for k in range(3):
        ppb[k] = part[:, k * 128 : (k + 1) * 128]
    ppb[3, :, 0 : M - 384] = part[:, 384:M]
    pl.semaphore_wait(barrier, NZ + NX + NL - 3)
    for i in range(1, NL):
        send(ppb.at[y_peer(i)], prs.at[i - 1], 0, (me, y_peer(i)))
    for i in range(1, NL):
        send(ids_ref, idr.at[lv], 1, (me, y_peer(i)))
    idr[lv] = ids_ref[...]

    load_m2l.wait()
    tms[:, 384:512] = jnp.zeros((128, 128), F32)
    for c in range(4):
        tms[c * 32 : (c + 1) * 32, 0:M] = dot(local, m2l[c])
    own = jnp.broadcast_to(meta[0:1, :].astype(F32), (128, 128))
    place = jnp.broadcast_to(meta[1:2, :].astype(F32), (128, 128)).T
    sub, lane = iota((128, 128), 0), iota((128, 128), 1)
    rank = jnp.sum(jnp.where((own.T == own) & (sub < lane), 1.0, 0.0), axis=0, keepdims=True)
    pos = (meta[0:1, :] * 2 + rank.astype(jnp.int32)) * 4
    keys = jnp.concatenate([pos + j for j in range(4)], axis=1)
    flat = tms[...]
    pieces = []
    for j in range(4):
        piece = flat if j == 0 else pltpu.roll(flat, 512 - CH * j, 1)
        piece = jnp.where(lane < CH, piece[:, 0:128], jnp.where(lane == 127, place + 1.0, 0.0))
        pieces.append(piece.astype(BF16))
    pieces = jnp.concatenate(pieces, axis=0)
    for q in range(4):
        hits = one_hot(iota((256, 512), 0) + q * 256 == keys)
        sb[q * 4 : (q + 1) * 4] = dot(hits, pieces).reshape(4, 8, 8, 128).astype(BF16)
    rb[15] = sb[zi]

    arrived(prs, 0)
    mine = ppb[lv] + prs[0] + prs[1] + prs[2]
    gz[zi] = mine.astype(BF16)

    def gather_z(k, c):
        send(gz.at[zi], gz.at[zi], 2, (z_peer(8 - k) * NX + xi, lv))
        return c

    def gather_z2(k, c):
        send(gz.at[zi], gz.at[zi], 2, (z_peer(8 + k) * NX + xi, lv))
        return c

    lax.fori_loop(0, 8, gather_z, 0)
    lax.fori_loop(1, 8, gather_z2, 0)

    def leaf_z(k, c):
        send(sb.at[z_peer(8 - k)], rb.at[2 * k], 3, (z_peer(8 - k) * NX + xi, lv))
        send(sb.at[z_peer(8 + k)], rb.at[2 * k - 1], 3, (z_peer(8 + k) * NX + xi, lv))
        return c

    send(sb.at[z_peer(8)], rb.at[0], 3, (z_peer(8) * NX + xi, lv))
    lax.fori_loop(1, 8, leaf_z, 0)

    row8 = iota((8, 128), 0)
    lane_t = iota((64, 128), 1)

    def near(m, carry):
        turned = pltpu.roll(tn[...], 128 - m, 1)
        columns = []
        for b2 in range(2):
            box = 2 * m + b2
            sources = []
            for pair in range(2):
                n1, n2 = 2 * pair, 2 * pair + 1
                d1, d2 = near_dir[box, n1], near_dir[box, n2]
                moved = jnp.where(low, tab[near_box[box, n1]], tab[near_box[box, n2]])
                parts = [(d // 9 - 1, lax.rem(d // 3, 3) - 1, lax.rem(d, 3) - 1) for d in (d1, d2)]
                shift = jnp.zeros((8, 128), F32)
                for c in range(3):
                    both = jnp.where(low, parts[0][c].astype(F32), parts[1][c].astype(F32))
                    shift = jnp.where(row8 == c, both, shift)
                moved = moved + shift
                sources.append([jnp.broadcast_to(moved[c : c + 1, :], (8, 128)) for c in range(6)])
            sums = [[], [], []]
            for tv in range(8):
                at = b2 * 64 + tv * 8
                x = [
                    jnp.broadcast_to(turned[at : at + 8, 16 * c : 16 * c + 1], (8, 128))
                    for c in range(3)
                ]
                acc = [jnp.zeros((8, 128), F32) for _ in range(3)]
                for pair in range(2):
                    src = sources[pair]
                    r = [x[c] - src[c] for c in range(3)]
                    t = r[0] * r[0] + r[1] * r[1] + r[2] * r[2] + EPS
                    inv = lax.rsqrt(t)
                    w = inv * inv * inv
                    q = w * (t + EPS)
                    wd = w * (r[0] * src[3] + r[1] * src[4] + r[2] * src[5])
                    for c in range(3):
                        acc[c] = acc[c] + (q * src[3 + c] + wd * r[c])
                column = [jnp.sum(acc[c], axis=1, keepdims=True) for c in range(3)]
                columns.append(
                    jnp.where(
                        iota((8, 128), 1) == 0,
                        column[0],
                        jnp.where(iota((8, 128), 1) == 1, column[1], column[2]),
                    )
                )
        turned_back = jnp.concatenate(columns, axis=0).T
        for c in range(3):
            nn[c, pl.ds(m, 1), :] = turned_back[c : c + 1, :]
        return carry

    lax.fori_loop(0, 16, near, 0)

    load_cm.wait()
    wt[...] = jnp.zeros((512, 512), F32)
    wt[0:M, 0:M] = cm[...]
    cmt[...] = wt[...].T.astype(BF16)

    arrived(gz.at[pl.ds(0, NZ - 1)], 2)
    for i in range(1, NX):
        send(gz, pall.at[xi], 4, (zi * NX + x_peer(i), lv))
    pall[xi] = gz[...]
    arrived(idr.at[pl.ds(0, NL - 1)], 1)
    parents = iota((8, 1024), 0)
    wanted = jnp.where(parents < 4, me * 4 + parents, -2)
    selects = []
    for l in range(NL):
        for c in range(4):
            selects.append(jnp.where(idr[l, c : c + 1, :] == wanted, 1.0, 0.0))
    select = jnp.concatenate(selects, axis=0).astype(BF16)
    arrived(pall.at[pl.ds(0, NX - 1)], 4)
    coarse = pall[...].astype(F32).reshape(1024, 128).astype(BF16)
    spb[...] = dot(select, coarse).reshape(4, 32, 128).astype(BF16)
    for i in range(1, NL):
        send(spb.at[y_peer(i)], spr.at[lv], 5, (me, y_peer(i)))
    spr[lv] = spb[lv]

    arrived(rb.at[pl.ds(0, NZ - 1)], 3)
    for i in range(1, NX):
        send(rb.at[:, x_peer(i)], fin.at[i - 1], 6, (zi * NX + x_peer(i), lv))
    fin[7] = rb[:, xi]

    arrived(spr.at[pl.ds(0, NL - 1)], 5)
    rows = jnp.concatenate([spr[k].astype(F32) for k in range(4)], axis=1)
    part = jnp.zeros((8, M), F32)
    for c in range(4):
        part = part + dot(rows[c * 8 : (c + 1) * 8, 0:M].astype(BF16), m2l[c])
    cpb[...] = 0.5 * part
    for i in range(1, NL):
        send(cpb, cpr.at[i - 1], 7, (me, y_peer(i)))
    arrived(cpr, 7)
    parent = cpb[...] + cpr[0] + cpr[1] + cpr[2]

    def box_of(lanes):
        beta = lax.rem(lanes, 32)
        return 2 * lax.rem(beta, 16) + beta // 16

    p_box = box_of(iota((8, 128), 1))
    lowered = jnp.zeros((M, 128), F32)
    for o in range(2):
        spread = one_hot((p_box // 8 == row8) & (lax.rem(p_box, 8) == lv * 2 + o))
        lowered = lowered + dot(child[o], dot(parent.astype(BF16), spread, ((0,), (0,))).astype(BF16))

    arrived(fin.at[pl.ds(0, NX - 1)], 6)
    got = fin[...].astype(F32).reshape(1024, 128)
    ident = got[:, 127:128]
    quarter = lax.rem(iota((1024, 1), 0), 4).astype(F32)
    key = jnp.where(ident > 0.5, ident - 1.0 + 32.0 * quarter, -1.0)
    landing = one_hot(key.astype(jnp.int32) == iota((1024, 128), 1))
    landed = dot(got.astype(BF16), landing, ((0,), (0,))).astype(BF16)
    e_box = box_of(lane)
    totals = [dot(landed[0:CH, :], one_hot(sub == 32 * j + e_box)) for j in range(4)]
    total = jnp.concatenate(totals, axis=0)[0:M, :] + lowered
    fl[...] = dot(cmt[0:M, 0:M], total.astype(BF16))

    def from_surface(i, carry):
        x = [jnp.broadcast_to(xg[c, pl.ds(i, 1), :], (8, 128)) for c in range(3)]
        acc = [jnp.zeros((8, 128), F32) for _ in range(3)]
        for kb in range(K // 8):
            at = kb * 8
            f = [fl[c * K + at : c * K + at + 8, :] for c in range(3)]
            r = [x[c] - shell[c * K + at : c * K + at + 8, :] for c in range(3)]
            q = qst[i, at : at + 8, :]
            wd = wst[i, at : at + 8, :] * (r[0] * f[0] + r[1] * f[1] + r[2] * f[2])
            for c in range(3):
                acc[c] = acc[c] + (q * f[c] + wd * r[c])
        for c in range(3):
            fo[pl.ds(c * 16 + i, 1), :] = jnp.sum(acc[c], axis=0, keepdims=True)
        return carry

    fo[48:128] = jnp.zeros((80, 128), F32)
    lax.fori_loop(0, 16, from_surface, 0)
    back = fo[...].T
    for c in range(3):
        total = jnp.zeros((16, 128), F32)
        for b2 in range(2):
            for g in range(4):
                at = g * 32 + b2 * 16
                pos = b2 * 4 + g
                piece = pltpu.roll(back[at : at + 16, :], (16 * (pos - c)) % 128, 1)
                total = jnp.where(lane16 == pos, piece, total)
        frb[c] = total + nn[c]
    for i in range(1, NL):
        send(frb, frr.at[i - 1], 8, (me, y_peer(i)))
    arrived(frr, 8)
    out_ref[...] = frb[...] + frr[0] + frr[1] + frr[2]

    gone(ppb.at[pl.ds(0, NL - 1)], 0)
    gone(idr.at[pl.ds(0, NL - 1)], 1)
    gone(gz.at[pl.ds(0, NZ - 1)], 2)
    gone(rb.at[pl.ds(0, NZ - 1)], 3)
    gone(pall.at[pl.ds(0, NX - 1)], 4)
    gone(spb.at[pl.ds(0, NL - 1)], 5)
    gone(fin.at[pl.ds(0, NX - 1)], 6)
    gone(cpr, 7)
    gone(frr, 8)


def local_part(
    offsets, vel_cot, m2l_ops, child_ops, check_map, leaf_dest, leaf_slot, coarse_dest,
    coarse_slot, near_box, near_dir,
):
    shell = jnp.asarray(np.repeat(surface_points().reshape(M, 1), 128, axis=1))
    ids = (coarse_dest[0, :, :, 0] * 4 + coarse_slot[0]).reshape(NZ, NX, 4, 4)
    ids = ids.transpose(3, 1, 0, 2)
    ids = jnp.pad(ids, ((0, 4), (0, 0), (0, 0), (0, 4)), constant_values=-1).reshape(8, 1024)
    meta = jnp.stack([leaf_dest[0, :, :, 0].T.reshape(128), leaf_slot[0].T.reshape(128)])
    vmem = pl.BlockSpec(memory_space=pltpu.VMEM)
    hbm = pl.BlockSpec(memory_space=pl.ANY)
    smem = pl.BlockSpec(memory_space=pltpu.SMEM)
    V = pltpu.VMEM
    out = pl.pallas_call(
        kernel,
        out_shape=jax.ShapeDtypeStruct((3, 16, 128), F32),
        in_specs=[vmem, vmem, hbm, hbm, hbm, vmem, vmem, vmem, smem, smem],
        out_specs=vmem,
        scratch_shapes=[
            V((4, M, M), BF16), V((2, M, M), BF16), V((M, M), F32), V((512, 512), BF16),
            V((8, 2048), F32), V((128, 128), F32), V((128, 128), F32), V((32, 8, 128), F32),
            V((6, 16, 128), F32), V((16, K, 128), F32), V((16, K, 128), F32), V((M, 128), F32),
            V((4, 8, 128), F32), V((3, 8, 128), F32), V((4, 8, 1024), jnp.int32),
            V((NZ, 8, 128), BF16), V((NX, NZ, 8, 128), BF16), V((4, 32, 128), BF16),
            V((4, 32, 128), BF16), V((8, M), F32), V((3, 8, M), F32), V((128, 512), F32),
            V((NZ, NX, 8, 128), BF16), V((NZ, NX, 8, 128), BF16), V((NX, NZ, 8, 128), BF16),
            V((512, 512), F32), V((M, 128), F32), V((3, 16, 128), F32), V((128, 128), F32),
            V((3, 16, 128), F32), V((3, 3, 16, 128), F32),
            pltpu.SemaphoreType.DMA((3,)), pltpu.SemaphoreType.DMA((9,)),
            pltpu.SemaphoreType.DMA((9,)),
        ],
        compiler_params=pltpu.CompilerParams(collective_id=0, has_side_effects=True),
    )(offsets, vel_cot, m2l_ops, child_ops, check_map, ids, meta, shell, near_box, near_dir)
    return out.reshape(3, 2048)


def solution(mesh):
    return jax.shard_map(
        local_part,
        mesh=mesh,
        in_specs=(
            P(None, "leaf"), P(None, "leaf"), P("lvl", None, None), P("lvl", None, None), P(),
            P("lvl", "leaf", None, None), P("lvl", "leaf", None), P("lvl", None, None, None),
            P("lvl", None, None), P("leaf", "lvl"), P("leaf", "lvl"),
        ),
        out_specs=P(None, "leaf"),
        check_vma=False,
    )
```

```python
import jax
import jax.numpy as jnp
import numpy as np
from jax import lax
from jax.experimental import pallas as pl
from jax.experimental.pallas import tpu as pltpu
from jax.sharding import PartitionSpec as P

SIDE = 6
EPS = 0.01
RADIUS = 0.525
M = 456
K = 152
NZ, NX, NL = 16, 8, 4
CH = 120
NEAREST = 2
F32, BF16, I32 = jnp.float32, jnp.bfloat16, jnp.int32
MESH = pl.DeviceIdType.MESH


def surface_points():
    levels = np.linspace(-1.0, 1.0, SIDE)
    lattice = np.stack(np.meshgrid(levels, levels, levels, indexing="ij"), 0).reshape(3, -1)
    on_shell = np.max(np.abs(lattice), 0) > 1.0 - 1e-09
    return (lattice[:, on_shell] * RADIUS).astype(np.float32)


def iota(shape, dim):
    return lax.broadcasted_iota(jnp.int32, shape, dim)


def dot(a, b, dims=((1,), (0,))):
    return lax.dot_general(a, b, (dims, ((), ())), preferred_element_type=F32)


def one_hot(hits):
    return jnp.where(hits, 1.0, 0.0).astype(BF16)


def kernel(
    off_h, vel_h, shell_h, leaf_dest_h, leaf_slot_h, coarse_dest_h, coarse_slot_h, near_box_h,
    near_dir_h, child_h, m2l_h, cm_h, out_ref,
    off, vel, shell, leaf_dest, leaf_slot, coarse_dest, coarse_slot, near_box, near_dir,
    m2l, child, cm, cmt, down, x6, nat, tn, thirds, tab, xg, wst, qst, av, ppb, prs, ids, gz, pall, spb, spr,
    cpb, cpr, meta, tms, sb, rb, fin, wt, fl, nn, fo, frb, frs, frr,
    loc, ss, rs,
):
    me, lv = lax.axis_index("leaf"), lax.axis_index("lvl")
    zi, xi = me // NX, lax.rem(me, NX)

    def z_peer(k):
        return lax.rem(zi + k, NZ)

    def x_peer(k):
        return lax.rem(xi + k, NX)

    def y_peer(k):
        return lax.rem(lv + k, NL)

    barrier = pltpu.get_barrier_semaphore()

    def greet_z(k, c):
        pl.semaphore_signal(barrier, 1, device_id=(z_peer(k) * NX + xi, lv), device_id_type=MESH)
        return c

    def greet_x(k, c):
        pl.semaphore_signal(barrier, 1, device_id=(zi * NX + x_peer(k), lv), device_id_type=MESH)
        return c

    def greet_y(k, c):
        pl.semaphore_signal(barrier, 1, device_id=(me, y_peer(k)), device_id_type=MESH)
        return c

    lax.fori_loop(1, NZ, greet_z, 0)
    lax.fori_loop(1, NX, greet_x, 0)
    lax.fori_loop(1, NL, greet_y, 0)

    loads = [
        pltpu.make_async_copy(src, dst, loc.at[n])
        for n, (src, dst) in enumerate(
            (
                (off_h, off), (vel_h, vel), (shell_h, shell), (leaf_dest_h, leaf_dest),
                (leaf_slot_h, leaf_slot), (coarse_dest_h, coarse_dest),
                (coarse_slot_h, coarse_slot), (near_box_h, near_box), (near_dir_h, near_dir),
                (child_h, child), (m2l_h, m2l), (cm_h, cm),
            )
        )
    ]
    for load in loads:
        load.start()

    def send(src, dst, phase, device):
        pltpu.make_async_remote_copy(
            src_ref=src, dst_ref=dst, send_sem=ss.at[phase], recv_sem=rs.at[phase],
            device_id=device, device_id_type=MESH,
        ).start()

    def arrived(ref, phase):
        pltpu.make_async_copy(ref, ref, rs.at[phase]).wait()

    def gone(ref, phase):
        pltpu.make_async_copy(ref, ref, ss.at[phase]).wait()

    groups = ((0, 6), (6, 6), (12, 4))

    def group_of(slot):
        return 3 if slot < 6 else 9 if slot < 12 else 10

    def forward(g):
        first, count = groups[g]
        arrived(rb.at[pl.ds(first, count - (g == 2))], group_of(first))
        for i in range(1, NX):
            src, dst = rb.at[pl.ds(first, count), x_peer(i)], fin.at[i - 1, pl.ds(first, count)]
            send(src, dst, 11 if g == 2 else 6, (zi * NX + x_peer(i), lv))

    for load in loads[0:3]:
        load.wait()
    x6[0:3] = off[...]
    x6[3:6] = vel[...]
    x6[6:8] = jnp.zeros((2, 2048), F32)
    low = iota((8, 128), 1) < 64
    for m in range(16):
        v = x6[:, m * 128 : (m + 1) * 128]
        nat[pl.ds(m, 8, stride=16), :] = v
        r = pltpu.roll(v, 64, 1)
        tab[2 * m] = jnp.where(low, v, r)
        tab[2 * m + 1] = jnp.where(low, r, v)
    tn[...] = nat[...].T
    lane16 = iota((16, 128), 1) // 16
    for c in range(3):
        whole = tn[...] if c == 0 else pltpu.roll(tn[...], 128 - 16 * c, 1)
        whole = jnp.where(iota((128, 128), 1) < 16, whole, 0.0)
        high = whole.astype(BF16).astype(F32)
        middle = (whole - high).astype(BF16).astype(F32)
        lowest = whole - high - middle
        split = high + pltpu.roll(middle, 16, 1) + pltpu.roll(lowest, 32, 1)
        thirds[c * 128 : (c + 1) * 128, :] = split.astype(BF16)
    for c in range(6):
        total = jnp.zeros((16, 128), F32)
        for b2 in range(2):
            for g in range(4):
                j, pos = b2 * 4 + g, g * 2 + b2
                piece = pltpu.roll(tn[16 * j : 16 * j + 16, :], (16 * (pos - c)) % 128, 1)
                total = jnp.where(lane16 == pos, piece, total)
        xg[c] = total

    def to_surface(kb, carry):
        row = pl.multiple_of(kb * 8, 8)
        s = [shell[pl.ds(c * K + row, 8), :] for c in range(3)]
        acc = [jnp.zeros((8, 128), F32) for _ in range(3)]
        for i in range(16):
            r = [s[c] - xg[c, i : i + 1, :] for c in range(3)]
            v = [xg[3 + c, i : i + 1, :] for c in range(3)]
            t = r[0] * r[0] + r[1] * r[1] + r[2] * r[2] + EPS
            inv = lax.rsqrt(t)
            w = inv * inv * inv
            q = w * (t + EPS)
            wd = w * (r[0] * v[0] + r[1] * v[1] + r[2] * v[2])
            for c in range(3):
                acc[c] = acc[c] + (q * v[c] + wd * r[c])
            wst[i, pl.ds(row, 8), :] = w
            qst[i, pl.ds(row, 8), :] = q
        for c in range(3):
            av[pl.ds(c * K + row, 8), :] = acc[c]
        return carry

    lax.fori_loop(0, K // 8, to_surface, 0)
    a = av[...]
    a = a + pltpu.roll(a, 64, 1)
    a = a + pltpu.roll(a, 32, 1)
    b_row, b_lane = iota((32, 128), 0), iota((32, 128), 1)
    pick = one_hot(b_lane == lax.rem(b_row, 2) * 16 + b_row // 2)
    local = dot(pick, a.astype(BF16), ((1,), (1,))).astype(BF16)

    for load in loads[3:7]:
        load.wait()
    for c in range(4):
        ids[lv, c : c + 1, :] = coarse_dest[c].astype(F32)
    ids[lv, 4:8, :] = coarse_slot[...].astype(F32)
    meta[...] = jnp.zeros((8, 128), F32)
    for c in range(4):
        meta[c : c + 1, 0:32] = leaf_dest[c].astype(F32)
    meta[4:8, 0:32] = leaf_slot[...].astype(F32)

    p_row, c_col = iota((8, 32), 0), iota((8, 32), 1)
    loads[9].wait()
    part = jnp.zeros((8, M), F32)
    for o in range(2):
        rows = one_hot((c_col == p_row * 8 + lv * 2 + o) & (p_row < 4))
        part = part + dot(dot(rows, local).astype(BF16), child[o])
    ppb[3] = jnp.zeros((8, 128), F32)
    for k in range(3):
        ppb[k] = part[:, k * 128 : (k + 1) * 128]
    ppb[3, :, 0 : M - 384] = part[:, 384:M]
    pl.semaphore_wait(barrier, NZ + NX + NL - 3)
    for i in range(1, NL):
        send(ppb.at[y_peer(i)], prs.at[i - 1], 0, (me, y_peer(i)))
    for i in range(1, NL):
        send(ids.at[lv], ids.at[lv], 1, (me, y_peer(i)))

    loads[10].wait()
    tms[:, 384:512] = jnp.zeros((128, 128), F32)
    for c in range(4):
        tms[c * 32 : (c + 1) * 32, 0:M] = dot(local, m2l[c])
    lane32 = iota((1, 128), 1) // 32
    listed = []
    for first in (0, 4):
        line = meta[first : first + 1, :]
        for c in range(1, 4):
            line = jnp.where(lane32 == c, pltpu.roll(meta[first + c : first + c + 1, :], 32 * c, 1), line)
        listed.append(line)
    own = jnp.broadcast_to(listed[0], (128, 128))
    place = jnp.broadcast_to(listed[1], (128, 128)).T
    sub, lane = iota((128, 128), 0), iota((128, 128), 1)
    rank = jnp.sum(jnp.where((own.T == own) & (sub < lane), 1.0, 0.0), axis=0, keepdims=True)
    pos = (listed[0] * 2.0 + rank).astype(jnp.int32) * 4
    keys = jnp.concatenate([pos + j for j in range(4)], axis=1)
    flat = tms[...]
    pieces = []
    for j in range(4):
        piece = flat if j == 0 else pltpu.roll(flat, 512 - CH * j, 1)
        piece = jnp.where(lane < CH, piece[:, 0:128], jnp.where(lane == 127, place + 1.0, 0.0))
        pieces.append(piece.astype(BF16))
    pieces = jnp.concatenate(pieces, axis=0)
    for q in range(4):
        hits = one_hot(iota((256, 512), 0) + q * 256 == keys)
        sb[q * 4 : (q + 1) * 4] = dot(hits, pieces).reshape(4, 8, 8, 128).astype(BF16)
    rb[15] = sb[zi]

    def leaf_z(first, last):
        for slot in range(first, last):
            k = 1 + slot // 2 if slot % 2 == 0 else NZ - 1 - slot // 2
            send(sb.at[z_peer(k)], rb.at[slot], group_of(slot), (z_peer(k) * NX + xi, lv))

    leaf_z(0, NEAREST)

    arrived(prs, 0)
    mine = ppb[lv] + prs[0] + prs[1] + prs[2]
    gz[4] = mine[0:4].astype(BF16)
    for k in (8, 7, 9, 6, 10, 5, 11, 4, 12, 3, 13, 2, 14, 1, 15):
        slot = (4 - k) % NZ
        send(gz.at[4], gz.at[slot], 2 if slot < 9 else 12, (z_peer(k) * NX + xi, lv))
    leaf_z(NEAREST, 15)

    row8 = iota((8, 128), 0)
    loads[7].wait()
    loads[8].wait()

    def digits(code):
        by9, by3 = (code * 57) >> 9, (code * 43) >> 7
        return by9 - 1, by3 - 3 * by9 - 1, code - 3 * by3 - 1

    def near(m, carry):
        chosen = one_hot(lax.rem(iota((48, 128), 0), 16) == m)
        targets = dot(thirds[:, 0:48], chosen)
        columns = [[], [], []]
        for b2 in range(2):
            box = 2 * m + b2
            sources = []
            for pair in range(2):
                n1, n2 = 2 * pair, 2 * pair + 1
                d1, d2 = near_dir[n1, box], near_dir[n2, box]
                moved = jnp.where(low, tab[near_box[n1, box]], tab[near_box[n2, box]])
                parts = [digits(d) for d in (d1, d2)]
                shift = jnp.zeros((8, 128), F32)
                for c in range(3):
                    both = jnp.where(low, parts[0][c].astype(F32), parts[1][c].astype(F32))
                    shift = jnp.where(row8 == c, both, shift)
                moved = moved + shift
                sources.append([jnp.broadcast_to(moved[c : c + 1, :], (8, 128)) for c in range(6)])
            for tv in range(8):
                at = b2 * 64 + tv * 8
                x = [targets[c * 128 + at : c * 128 + at + 8, :] for c in range(3)]
                acc = [jnp.zeros((8, 128), F32) for _ in range(3)]
                for src in sources:
                    r = [x[c] - src[c] for c in range(3)]
                    t = r[0] * r[0] + r[1] * r[1] + r[2] * r[2] + EPS
                    inv = lax.rsqrt(t)
                    w = inv * inv * inv
                    q = w * (t + EPS)
                    wd = w * (r[0] * src[3] + r[1] * src[4] + r[2] * src[5])
                    for c in range(3):
                        acc[c] = acc[c] + (q * src[3 + c] + wd * r[c])
                for c in range(3):
                    columns[c].append(acc[c])
        for c in range(3):
            total = jnp.concatenate(columns[c], axis=0)
            high = total.astype(BF16)
            rest = (total - high.astype(F32)).astype(BF16)
            both = jnp.concatenate([high, rest], axis=1)
            nn[c, pl.ds(m, 1), :] = dot(jnp.ones((8, 256), BF16), both, ((1,), (1,)))[0:1, :]
        return carry

    lax.fori_loop(0, 16, near, 0, unroll=2)

    loads[11].wait()
    wt[...] = jnp.zeros((512, 512), F32)
    wt[0:M, 0:M] = cm[...]
    cmt[...] = wt[...].T.astype(BF16)

    for first, count, phase in ((0, 9, 2), (9, 7, 12)):
        arrived(gz.at[pl.ds(first, min(count, 8))], phase)
        for i in range(1, NX):
            part = gz.at[pl.ds(first, count)]
            send(part, pall.at[xi, pl.ds(first, count)], 4, (zi * NX + x_peer(i), lv))
    pall[xi] = gz[...]
    for o in range(2):
        down[o] = dot(cmt[0:M, 0:M], child[o]).astype(BF16)
    arrived(ids.at[pl.ds(0, NL - 1)], 1)
    col = iota((512, 512), 1)
    plane = lax.rem(zi + lax.rem(col // 4, NZ) + 12, NZ)
    gathered = (plane * NX + col // 64) * 4 + lax.rem(col, 4)
    order = one_hot(iota((512, 512), 0) == gathered)
    listed = dot(ids[...].reshape(32, 512).astype(BF16), order)
    parents = iota((8, 512), 0)
    wanted = (me * 4 + lax.rem(parents, 4)).astype(F32)
    selects = []
    for l in range(NL):
        for c in (0, 2):
            first, second = (
                listed[8 * l + n : 8 * l + n + 1, :] * 4.0 + listed[8 * l + 4 + n : 8 * l + 5 + n, :]
                for n in (c, c + 1)
            )
            named = jnp.where(parents < 4, first, second)
            selects.append(jnp.where(named == wanted, 1.0, 0.0))
    select = jnp.concatenate(selects, axis=0).astype(BF16)
    forward(0)
    arrived(pall.at[pl.ds(0, NX - 1)], 4)
    coarse = [
        jnp.concatenate([pall[x, 2 * z].astype(F32), pall[x, 2 * z + 1].astype(F32)], axis=0)
        for x in range(NX)
        for z in range(NZ // 2)
    ]
    coarse = jnp.concatenate(coarse, axis=0).astype(BF16)
    spb[...] = dot(select, coarse).reshape(4, 16, 128).astype(BF16)
    for i in range(1, NL):
        send(spb.at[y_peer(i)], spr.at[lv], 5, (me, y_peer(i)))
    spr[lv] = spb[lv]

    forward(1)

    arrived(spr.at[pl.ds(0, NL - 1)], 5)
    rows = jnp.concatenate([spr[k].astype(F32) for k in range(4)], axis=1)[:, 0:M]
    part = jnp.zeros((16, M), F32)
    for c in range(4):
        part = part + dot(jnp.where(iota((16, M), 0) // 4 == c, rows, 0.0).astype(BF16), m2l[c])
    part = part[0:8] + part[8:16]
    cpb[...] = 0.5 * (part[0:4] + part[4:8])
    for i in range(1, NL):
        send(cpb, cpr.at[i - 1], 7, (me, y_peer(i)))
    forward(2)
    def box_of(lanes):
        beta = lax.rem(lanes, 32)
        return 2 * lax.rem(beta, 16) + beta // 16

    def landed(first, count, phase):
        fin[7, first : first + count] = rb[first : first + count, xi]
        arrived(fin.at[pl.ds(0, NX - 1), pl.ds(first, count)], phase)
        size = NX * count * 8
        got = fin[:, first : first + count].astype(F32).reshape(size, 128)
        ident = got[:, 127:128]
        quarter = lax.rem(iota((size, 1), 0), 4).astype(F32)
        key = jnp.where(ident > 0.5, ident - 1.0 + 32.0 * quarter, -1.0)
        landing = one_hot(key.astype(jnp.int32) == iota((size, 128), 1))
        return dot(got.astype(BF16), landing, ((0,), (0,)))

    leaf_sum = landed(0, 12, 6)
    arrived(cpr, 7)
    parent = jnp.concatenate([cpb[...] + cpr[0] + cpr[1] + cpr[2], jnp.zeros((4, M), F32)], axis=0)
    p_box = box_of(iota((8, 128), 1))
    lowered = jnp.zeros((M, 128), F32)
    for o in range(2):
        spread = one_hot((p_box // 8 == row8) & (lax.rem(p_box, 8) == lv * 2 + o))
        octant = dot(parent.astype(BF16), spread, ((0,), (0,))).astype(BF16)
        lowered = lowered + dot(down[o], octant)
    leaf_sum = (leaf_sum + landed(12, 4, 11)).astype(BF16)
    e_box = box_of(lane)
    totals = [dot(leaf_sum[0:CH, :], one_hot(sub == 32 * j + e_box)) for j in range(4)]
    total = jnp.concatenate(totals, axis=0)[0:M, :].astype(BF16)
    fl[...] = dot(cmt[0:M, 0:M], total) + lowered

    def from_surface(i, carry):
        x = [jnp.broadcast_to(xg[c, pl.ds(i, 1), :], (8, 128)) for c in range(3)]
        acc = [jnp.zeros((8, 128), F32) for _ in range(3)]
        for kb in range(K // 8):
            at = kb * 8
            f = [fl[c * K + at : c * K + at + 8, :] for c in range(3)]
            r = [x[c] - shell[c * K + at : c * K + at + 8, :] for c in range(3)]
            q = qst[i, at : at + 8, :]
            wd = wst[i, at : at + 8, :] * (r[0] * f[0] + r[1] * f[1] + r[2] * f[2])
            for c in range(3):
                acc[c] = acc[c] + (q * f[c] + wd * r[c])
        for c in range(3):
            fo[pl.ds(c * 16 + i, 1), :] = jnp.sum(acc[c], axis=0, keepdims=True)
        return carry

    fo[48:128] = jnp.zeros((80, 128), F32)
    lax.fori_loop(0, 16, from_surface, 0)
    back = fo[...].T
    for c in range(3):
        total = jnp.zeros((16, 128), F32)
        for b2 in range(2):
            for g in range(4):
                at = g * 32 + b2 * 16
                pos = b2 * 4 + g
                piece = pltpu.roll(back[at : at + 16, :], (16 * (pos - c)) % 128, 1)
                total = jnp.where(lane16 == pos, piece, total)
        frb[c] = total + nn[c]
    frs[...] = frb[...].astype(BF16)
    for i in range(1, NL):
        send(frs, frr.at[i - 1], 8, (me, y_peer(i)))
    arrived(frr, 8)
    forces = frb[...] + frr[0].astype(F32) + frr[1].astype(F32) + frr[2].astype(F32)
    for c in range(3):
        for m in range(16):
            out_ref[c : c + 1, m * 128 : (m + 1) * 128] = forces[c, m : m + 1, :]

    gone(ppb.at[pl.ds(0, NL - 1)], 0)
    gone(ids.at[pl.ds(0, NL - 1)], 1)
    gone(gz.at[pl.ds(0, 8)], 2)
    gone(gz.at[pl.ds(0, 7)], 12)
    gone(rb.at[pl.ds(0, 6)], 3)
    gone(rb.at[pl.ds(0, 6)], 9)
    gone(rb.at[pl.ds(0, 3)], 10)
    gone(pall.at[pl.ds(0, NX - 1)], 4)
    gone(spb.at[pl.ds(0, NL - 1)], 5)
    gone(fin.at[pl.ds(0, NX - 1), pl.ds(0, 12)], 6)
    gone(fin.at[pl.ds(0, NX - 1), pl.ds(0, 4)], 11)
    gone(cpr, 7)
    gone(frr, 8)


def local_part(
    offsets, vel_cot, m2l_ops, child_ops, check_map, leaf_dest, leaf_slot, coarse_dest,
    coarse_slot, near_box, near_dir,
):
    shell = jnp.asarray(np.repeat(surface_points().reshape(M, 1), 128, axis=1))
    vmem = pl.BlockSpec(memory_space=pltpu.VMEM)
    hbm = pl.BlockSpec(memory_space=pl.ANY)
    V = pltpu.VMEM
    return pl.pallas_call(
        kernel,
        out_shape=jax.ShapeDtypeStruct((3, 2048), F32),
        in_specs=[hbm] * 12,
        out_specs=vmem,
        scratch_shapes=[
            V((3, 2048), F32), V((3, 2048), F32), V((M, 128), F32), V((4, 1, 32), I32),
            V((4, 32), I32), V((4, 1, 512), I32), V((4, 512), I32), pltpu.SMEM((4, 32), I32),
            pltpu.SMEM((4, 32), I32),
            V((4, M, M), BF16), V((2, M, M), BF16), V((M, M), F32), V((512, 512), BF16),
            V((2, M, M), BF16),
            V((8, 2048), F32), V((128, 128), F32), V((128, 128), F32), V((384, 128), BF16), V((32, 8, 128), F32),
            V((6, 16, 128), F32), V((16, K, 128), F32), V((16, K, 128), F32), V((M, 128), F32),
            V((4, 8, 128), F32), V((3, 8, 128), F32), V((4, 8, 512), F32),
            V((NZ, 4, 128), BF16), V((NX, NZ, 4, 128), BF16), V((4, 16, 128), BF16),
            V((4, 16, 128), BF16), V((4, M), F32), V((3, 4, M), F32), V((8, 128), F32), V((128, 512), F32),
            V((NZ, NX, 8, 128), BF16), V((NZ, NX, 8, 128), BF16), V((NX, NZ, 8, 128), BF16),
            V((512, 512), F32), V((M, 128), F32), V((3, 16, 128), F32), V((128, 128), F32),
            V((3, 16, 128), F32), V((3, 16, 128), BF16), V((3, 3, 16, 128), BF16),
            pltpu.SemaphoreType.DMA((12,)), pltpu.SemaphoreType.DMA((13,)),
            pltpu.SemaphoreType.DMA((13,)),
        ],
        compiler_params=pltpu.CompilerParams(collective_id=0, has_side_effects=True),
    )(
        offsets, vel_cot, shell, leaf_dest[0].transpose(1, 2, 0), leaf_slot[0].T,
        coarse_dest[0].transpose(1, 2, 0), coarse_slot[0].T, near_box.T, near_dir.T, child_ops,
        m2l_ops, check_map,
    )


def solution(mesh):
    return jax.shard_map(
        local_part,
        mesh=mesh,
        in_specs=(
            P(None, "leaf"), P(None, "leaf"), P("lvl", None, None), P("lvl", None, None), P(),
            P("lvl", "leaf", None, None), P("lvl", "leaf", None), P("lvl", None, None, None),
            P("lvl", None, None), P("leaf", "lvl"), P("leaf", "lvl"),
        ),
        out_specs=P(None, "leaf"),
        check_vma=False,
    )
```

```python
import jax
import jax.numpy as jnp
import numpy as np
from jax import lax
from jax.experimental import pallas as pl
from jax.experimental.pallas import tpu as pltpu
from jax.sharding import PartitionSpec as P

SIDE = 6
EPS = 0.01
RADIUS = 0.525
M = 456
K = 152
NZ, NX, NL = 16, 8, 4
CH = 120
NEAREST = 4
F32, BF16, I32 = jnp.float32, jnp.bfloat16, jnp.int32
MESH = pl.DeviceIdType.MESH


def surface_points():
    levels = np.linspace(-1.0, 1.0, SIDE)
    lattice = np.stack(np.meshgrid(levels, levels, levels, indexing="ij"), 0).reshape(3, -1)
    on_shell = np.max(np.abs(lattice), 0) > 1.0 - 1e-09
    return (lattice[:, on_shell] * RADIUS).astype(np.float32)


def iota(shape, dim):
    return lax.broadcasted_iota(jnp.int32, shape, dim)


def dot(a, b, dims=((1,), (0,))):
    return lax.dot_general(a, b, (dims, ((), ())), preferred_element_type=F32)


def one_hot(hits):
    return jnp.where(hits, 1.0, 0.0).astype(BF16)


def kernel(
    off_h, vel_h, shell_h, leaf_dest_h, leaf_slot_h, coarse_dest_h, coarse_slot_h, near_box_h,
    near_dir_h, child_h, m2l_h, cm_h, own_ref, others_ref,
    off, vel, shell, leaf_dest, leaf_slot, coarse_dest, coarse_slot, near_box, near_dir,
    m2l, child, cm, cmt, down, x6, nat, tn, thirds, tab, xg, wst, qst, av, ppb, prs, ids, gz, pall, spb, spr,
    cpb, cpr, meta, tms, sb, rb, fin, wt, fl, nn, fo, frb, frs, frr,
    loc, ss, rs,
):
    me, lv = lax.axis_index("leaf"), lax.axis_index("lvl")
    zi, xi = me // NX, lax.rem(me, NX)

    def z_peer(k):
        return lax.rem(zi + k, NZ)

    def x_peer(k):
        return lax.rem(xi + k, NX)

    def y_peer(k):
        return lax.rem(lv + k, NL)

    barrier = pltpu.get_barrier_semaphore()

    def greet_z(k, c):
        pl.semaphore_signal(barrier, 1, device_id=(z_peer(k) * NX + xi, lv), device_id_type=MESH)
        return c

    def greet_x(k, c):
        pl.semaphore_signal(barrier, 1, device_id=(zi * NX + x_peer(k), lv), device_id_type=MESH)
        return c

    def greet_y(k, c):
        pl.semaphore_signal(barrier, 1, device_id=(me, y_peer(k)), device_id_type=MESH)
        return c

    loads = [
        pltpu.make_async_copy(src, dst, loc.at[n])
        for n, (src, dst) in enumerate(
            (
                (off_h, off), (vel_h, vel), (shell_h, shell), (leaf_dest_h, leaf_dest),
                (leaf_slot_h, leaf_slot), (coarse_dest_h, coarse_dest),
                (coarse_slot_h, coarse_slot), (near_box_h, near_box), (near_dir_h, near_dir),
                (child_h, child), (m2l_h, m2l), (cm_h, cm),
            )
        )
    ]
    for load in loads[0:3]:
        load.start()
    lax.fori_loop(1, NZ, greet_z, 0)
    lax.fori_loop(1, NX, greet_x, 0)
    lax.fori_loop(1, NL, greet_y, 0)
    for n in (9, 3, 4, 5, 6, 10, 7, 8, 11):
        loads[n].start()

    def send(src, dst, phase, device):
        pltpu.make_async_remote_copy(
            src_ref=src, dst_ref=dst, send_sem=ss.at[phase], recv_sem=rs.at[phase],
            device_id=device, device_id_type=MESH,
        ).start()

    def arrived(ref, phase):
        pltpu.make_async_copy(ref, ref, rs.at[phase]).wait()

    def gone(ref, phase):
        pltpu.make_async_copy(ref, ref, ss.at[phase]).wait()

    groups = ((0, 8), (8, 4), (12, 4))

    def group_of(slot):
        return 3 if slot < 8 else 9 if slot < 12 else 10

    def forward(g):
        first, count = groups[g]
        arrived(rb.at[pl.ds(first, count - (g == 2))], group_of(first))
        for i in (4, 3, 5, 2, 6, 1, 7):
            src, dst = rb.at[pl.ds(first, count), x_peer(i)], fin.at[i - 1, pl.ds(first, count)]
            send(src, dst, 11 if g == 2 else 6, (zi * NX + x_peer(i), lv))

    for load in loads[0:3]:
        load.wait()
    x6[0:3] = off[...]
    x6[3:6] = vel[...]
    x6[6:8] = jnp.zeros((2, 2048), F32)
    low = iota((8, 128), 1) < 64
    for m in range(16):
        v = x6[:, m * 128 : (m + 1) * 128]
        nat[pl.ds(m, 8, stride=16), :] = v
        r = pltpu.roll(v, 64, 1)
        tab[2 * m] = jnp.where(low, v, r)
        tab[2 * m + 1] = jnp.where(low, r, v)
    tn[...] = nat[...].T
    lane16 = iota((16, 128), 1) // 16
    for c in range(3):
        whole = tn[...] if c == 0 else pltpu.roll(tn[...], 128 - 16 * c, 1)
        whole = jnp.where(iota((128, 128), 1) < 16, whole, 0.0)
        high = whole.astype(BF16).astype(F32)
        middle = (whole - high).astype(BF16).astype(F32)
        lowest = whole - high - middle
        split = high + pltpu.roll(middle, 16, 1) + pltpu.roll(lowest, 32, 1)
        thirds[c * 128 : (c + 1) * 128, :] = split.astype(BF16)
    for c in range(6):
        total = jnp.zeros((16, 128), F32)
        for b2 in range(2):
            for g in range(4):
                j, pos = b2 * 4 + g, g * 2 + b2
                piece = pltpu.roll(tn[16 * j : 16 * j + 16, :], (16 * (pos - c)) % 128, 1)
                total = jnp.where(lane16 == pos, piece, total)
        xg[c] = total

    def to_surface(kb, carry):
        row = pl.multiple_of(kb * 8, 8)
        s = [shell[pl.ds(c * K + row, 8), :] for c in range(3)]
        acc = [jnp.zeros((8, 128), F32) for _ in range(3)]
        for i in range(16):
            r = [s[c] - xg[c, i : i + 1, :] for c in range(3)]
            v = [xg[3 + c, i : i + 1, :] for c in range(3)]
            t = r[0] * r[0] + r[1] * r[1] + r[2] * r[2] + EPS
            inv = lax.rsqrt(t)
            w = inv * inv * inv
            q = w * (t + EPS)
            wd = w * (r[0] * v[0] + r[1] * v[1] + r[2] * v[2])
            for c in range(3):
                acc[c] = acc[c] + (q * v[c] + wd * r[c])
            wst[i, pl.ds(row, 8), :] = w
            qst[i, pl.ds(row, 8), :] = q
        for c in range(3):
            av[pl.ds(c * K + row, 8), :] = acc[c]
        return carry

    lax.fori_loop(0, K // 8, to_surface, 0)
    a = av[...]
    a = a + pltpu.roll(a, 64, 1)
    a = a + pltpu.roll(a, 32, 1)
    b_row, b_lane = iota((32, 128), 0), iota((32, 128), 1)
    pick = one_hot(b_lane == lax.rem(b_row, 2) * 16 + b_row // 2)
    summed = a.astype(BF16)
    local = dot(pick, summed, ((1,), (1,))).astype(BF16)

    for load in loads[3:7]:
        load.wait()
    for c in range(4):
        ids[lv, c : c + 1, :] = coarse_dest[c].astype(F32)
    ids[lv, 4:8, :] = coarse_slot[...].astype(F32)
    meta[...] = jnp.zeros((8, 128), F32)
    for c in range(4):
        meta[c : c + 1, 0:32] = leaf_dest[c].astype(F32)
    meta[4:8, 0:32] = leaf_slot[...].astype(F32)

    p_row, p_lane = iota((8, 128), 0), iota((8, 128), 1)
    loads[9].wait()
    part = jnp.zeros((8, M), F32)
    for o in range(2):
        rows = one_hot((p_lane == o * 16 + p_row * 4 + lv) & (p_row < 4))
        part = part + dot(dot(rows, summed, ((1,), (1,))).astype(BF16), child[o])
    ppb[3] = jnp.zeros((4, 128), F32)
    for k in range(3):
        ppb[k] = part[0:4, k * 128 : (k + 1) * 128]
    ppb[3, :, 0 : M - 384] = part[0:4, 384:M]
    pl.semaphore_wait(barrier, NZ + NX + NL - 3)
    for i in range(1, NL):
        send(ppb.at[y_peer(i)], prs.at[i - 1], 0, (me, y_peer(i)))

    loads[10].wait()
    tms[:, 384:512] = jnp.zeros((128, 128), F32)
    for c in range(4):
        tms[c * 32 : (c + 1) * 32, 0:M] = dot(local, m2l[c])
    lane32 = iota((1, 128), 1) // 32
    listed = []
    for first in (0, 4):
        line = meta[first : first + 1, :]
        for c in range(1, 4):
            line = jnp.where(lane32 == c, pltpu.roll(meta[first + c : first + c + 1, :], 32 * c, 1), line)
        listed.append(line)
    own = jnp.broadcast_to(listed[0], (128, 128))
    place = jnp.broadcast_to(listed[1], (128, 128)).T
    sub, lane = iota((128, 128), 0), iota((128, 128), 1)
    rank = jnp.sum(jnp.where((own.T == own) & (sub < lane), 1.0, 0.0), axis=0, keepdims=True)
    pos = (listed[0] * 2.0 + rank).astype(jnp.int32) * 4
    keys = jnp.concatenate([pos + j for j in range(4)], axis=1)
    flat = tms[...]
    pieces = []
    for j in range(4):
        piece = flat if j == 0 else pltpu.roll(flat, 512 - CH * j, 1)
        piece = jnp.where(lane < CH, piece[:, 0:128], jnp.where(lane == 127, place + 1.0, 0.0))
        pieces.append(piece.astype(BF16))
    pieces = jnp.concatenate(pieces, axis=0)
    for q in range(4):
        hits = one_hot(iota((256, 512), 0) + q * 256 == keys)
        sb[q * 4 : (q + 1) * 4] = dot(hits, pieces).reshape(4, 8, 8, 128).astype(BF16)
    rb[15] = sb[zi]

    def leaf_z(first, last):
        for slot in range(first, last):
            k = 1 + slot // 2 if slot % 2 == 0 else NZ - 1 - slot // 2
            send(sb.at[z_peer(k)], rb.at[slot], group_of(slot), (z_peer(k) * NX + xi, lv))

    leaf_z(0, NEAREST)

    arrived(prs, 0)
    mine = ppb[lv] + prs[0] + prs[1] + prs[2]
    gz[4] = mine.astype(BF16)
    for k in (8, 7, 9, 6, 10, 5, 11, 4, 12, 3, 13, 2, 14, 1, 15):
        slot = (4 - k) % NZ
        send(gz.at[4], gz.at[slot], 2 if slot < 9 else 12, (z_peer(k) * NX + xi, lv))
    leaf_z(NEAREST, 15)
    for i in range(1, NL):
        send(ids.at[lv], ids.at[lv], 1, (me, y_peer(i)))

    row8 = iota((8, 128), 0)
    loads[7].wait()
    loads[8].wait()

    def digits(code):
        by9, by3 = (code * 57) >> 9, (code * 43) >> 7
        return by9 - 1, by3 - 3 * by9 - 1, code - 3 * by3 - 1

    def near(m, carry):
        chosen = one_hot(lax.rem(iota((48, 128), 0), 16) == m)
        targets = dot(thirds[:, 0:48], chosen)
        columns = [[], [], []]
        for b2 in range(2):
            box = 2 * m + b2
            sources = []
            for pair in range(2):
                n1, n2 = 2 * pair, 2 * pair + 1
                d1, d2 = near_dir[n1, box], near_dir[n2, box]
                moved = jnp.where(low, tab[near_box[n1, box]], tab[near_box[n2, box]])
                parts = [digits(d) for d in (d1, d2)]
                shift = jnp.zeros((8, 128), F32)
                for c in range(3):
                    both = jnp.where(low, parts[0][c].astype(F32), parts[1][c].astype(F32))
                    shift = jnp.where(row8 == c, both, shift)
                moved = moved + shift
                sources.append([jnp.broadcast_to(moved[c : c + 1, :], (8, 128)) for c in range(6)])
            for tv in range(8):
                at = b2 * 64 + tv * 8
                x = [targets[c * 128 + at : c * 128 + at + 8, :] for c in range(3)]
                acc = [jnp.zeros((8, 128), F32) for _ in range(3)]
                for src in sources:
                    r = [x[c] - src[c] for c in range(3)]
                    t = r[0] * r[0] + r[1] * r[1] + r[2] * r[2] + EPS
                    inv = lax.rsqrt(t)
                    w = inv * inv * inv
                    q = w * (t + EPS)
                    wd = w * (r[0] * src[3] + r[1] * src[4] + r[2] * src[5])
                    for c in range(3):
                        acc[c] = acc[c] + (q * src[3 + c] + wd * r[c])
                for c in range(3):
                    columns[c].append(acc[c])
        for c in range(3):
            total = jnp.concatenate(columns[c], axis=0)
            high = total.astype(BF16)
            rest = (total - high.astype(F32)).astype(BF16)
            both = jnp.concatenate([high, rest], axis=1)
            nn[c, pl.ds(m, 1), :] = dot(jnp.ones((8, 256), BF16), both, ((1,), (1,)))[0:1, :]
        return carry

    lax.fori_loop(0, 16, near, 0, unroll=2)

    loads[11].wait()
    wt[...] = jnp.zeros((512, 512), F32)
    wt[0:M, 0:M] = cm[...]
    cmt[...] = wt[...].T.astype(BF16)

    for first, count, phase in ((0, 9, 2), (9, 7, 12)):
        arrived(gz.at[pl.ds(first, min(count, 8))], phase)
        for i in (4, 3, 5, 2, 6, 1, 7):
            part = gz.at[pl.ds(first, count)]
            send(part, pall.at[xi, pl.ds(first, count)], 4, (zi * NX + x_peer(i), lv))
    pall[xi] = gz[...]
    for o in range(2):
        down[o] = dot(cmt[0:M, 0:M], child[o]).astype(BF16)
    arrived(ids.at[pl.ds(0, NL - 1)], 1)
    col = iota((512, 512), 1)
    plane = lax.rem(zi + lax.rem(col // 4, NZ) + 12, NZ)
    gathered = (plane * NX + col // 64) * 4 + lax.rem(col, 4)
    order = one_hot(iota((512, 512), 0) == gathered)
    listed = dot(ids[...].reshape(32, 512).astype(BF16), order)
    parents = iota((8, 512), 0)
    wanted = (me * 4 + lax.rem(parents, 4)).astype(F32)
    selects = []
    for l in range(NL):
        for c in (0, 2):
            first, second = (
                listed[8 * l + n : 8 * l + n + 1, :] * 4.0 + listed[8 * l + 4 + n : 8 * l + 5 + n, :]
                for n in (c, c + 1)
            )
            named = jnp.where(parents < 4, first, second)
            selects.append(jnp.where(named == wanted, 1.0, 0.0))
    select = jnp.concatenate(selects, axis=0).astype(BF16)
    forward(0)
    arrived(pall.at[pl.ds(0, NX - 1)], 4)
    coarse = [
        jnp.concatenate([pall[x, 2 * z].astype(F32), pall[x, 2 * z + 1].astype(F32)], axis=0)
        for x in range(NX)
        for z in range(NZ // 2)
    ]
    coarse = jnp.concatenate(coarse, axis=0).astype(BF16)
    spb[...] = dot(select, coarse).reshape(4, 16, 128).astype(BF16)
    for i in range(1, NL):
        send(spb.at[y_peer(i)], spr.at[lv], 5, (me, y_peer(i)))
    spr[lv] = spb[lv]

    forward(1)

    arrived(spr.at[pl.ds(0, NL - 1)], 5)
    rows = jnp.concatenate([spr[k].astype(F32) for k in range(4)], axis=1)[:, 0:M]
    part = jnp.zeros((16, M), F32)
    for c in range(4):
        part = part + dot(jnp.where(iota((16, M), 0) // 4 == c, rows, 0.0).astype(BF16), m2l[c])
    part = part[0:8] + part[8:16]
    cpb[...] = 0.5 * (part[0:4] + part[4:8])
    for i in range(1, NL):
        send(cpb, cpr.at[i - 1], 7, (me, y_peer(i)))
    forward(2)
    def box_of(lanes):
        beta = lax.rem(lanes, 32)
        return 2 * lax.rem(beta, 16) + beta // 16

    def landed(first, count, phase):
        fin[7, first : first + count] = rb[first : first + count, xi]
        arrived(fin.at[pl.ds(0, NX - 1), pl.ds(first, count)], phase)
        size = NX * count * 8
        got = fin[:, first : first + count].astype(F32).reshape(size, 128)
        ident = got[:, 127:128]
        quarter = lax.rem(iota((size, 1), 0), 4).astype(F32)
        key = jnp.where(ident > 0.5, ident - 1.0 + 32.0 * quarter, -1.0)
        landing = one_hot(key.astype(jnp.int32) == iota((size, 128), 1))
        return dot(got.astype(BF16), landing, ((0,), (0,)))

    leaf_sum = landed(0, 12, 6)
    arrived(cpr, 7)
    parent = jnp.concatenate([cpb[...] + cpr[0] + cpr[1] + cpr[2], jnp.zeros((4, M), F32)], axis=0)
    p_box = box_of(iota((8, 128), 1))
    lowered = jnp.zeros((M, 128), F32)
    for o in range(2):
        spread = one_hot((p_box // 8 == row8) & (lax.rem(p_box, 8) == lv * 2 + o))
        octant = dot(parent.astype(BF16), spread, ((0,), (0,))).astype(BF16)
        lowered = lowered + dot(down[o], octant)
    leaf_sum = (leaf_sum + landed(12, 4, 11)).astype(BF16)
    e_box = box_of(lane)
    totals = [dot(leaf_sum[0:CH, :], one_hot(sub == 32 * j + e_box)) for j in range(4)]
    total = jnp.concatenate(totals, axis=0)[0:M, :].astype(BF16)
    fl[...] = dot(cmt[0:M, 0:M], total) + lowered

    def from_surface(i, carry):
        x = [jnp.broadcast_to(xg[c, pl.ds(i, 1), :], (8, 128)) for c in range(3)]
        acc = [jnp.zeros((8, 128), F32) for _ in range(3)]
        for kb in range(K // 8):
            at = kb * 8
            f = [fl[c * K + at : c * K + at + 8, :] for c in range(3)]
            r = [x[c] - shell[c * K + at : c * K + at + 8, :] for c in range(3)]
            q = qst[i, at : at + 8, :]
            wd = wst[i, at : at + 8, :] * (r[0] * f[0] + r[1] * f[1] + r[2] * f[2])
            for c in range(3):
                acc[c] = acc[c] + (q * f[c] + wd * r[c])
        for c in range(3):
            fo[pl.ds(c * 16 + i, 1), :] = jnp.sum(acc[c], axis=0, keepdims=True)
        return carry

    fo[48:128] = jnp.zeros((80, 128), F32)
    lax.fori_loop(0, 16, from_surface, 0)
    back = fo[...].T
    for c in range(3):
        total = jnp.zeros((16, 128), F32)
        for b2 in range(2):
            for g in range(4):
                at = g * 32 + b2 * 16
                pos = b2 * 4 + g
                piece = pltpu.roll(back[at : at + 16, :], (16 * (pos - c)) % 128, 1)
                total = jnp.where(lane16 == pos, piece, total)
        frb[c] = total + nn[c]
    frs[...] = frb[...].astype(BF16)
    for i in range(1, NL):
        send(frs, frr.at[i - 1], 8, (me, y_peer(i)))

    def spread_out(ref, forces):
        for c in range(3):
            for m in range(16):
                ref[c : c + 1, m * 128 : (m + 1) * 128] = forces[c, m : m + 1, :]

    spread_out(own_ref, frb[...])
    arrived(frr, 8)
    spread_out(others_ref, frr[0].astype(F32) + frr[1].astype(F32) + frr[2].astype(F32))

    gone(ppb.at[pl.ds(0, NL - 1)], 0)
    gone(ids.at[pl.ds(0, NL - 1)], 1)
    gone(gz.at[pl.ds(0, 8)], 2)
    gone(gz.at[pl.ds(0, 7)], 12)
    gone(rb.at[pl.ds(0, 8)], 3)
    gone(rb.at[pl.ds(0, 4)], 9)
    gone(rb.at[pl.ds(0, 3)], 10)
    gone(pall.at[pl.ds(0, NX - 1)], 4)
    gone(spb.at[pl.ds(0, NL - 1)], 5)
    gone(fin.at[pl.ds(0, NX - 1), pl.ds(0, 12)], 6)
    gone(fin.at[pl.ds(0, NX - 1), pl.ds(0, 4)], 11)
    gone(cpr, 7)
    gone(frr, 8)


def local_part(
    offsets, vel_cot, m2l_ops, child_ops, check_map, leaf_dest, leaf_slot, coarse_dest,
    coarse_slot, near_box, near_dir,
):
    shell = jnp.asarray(np.repeat(surface_points().reshape(M, 1), 128, axis=1))
    vmem = pl.BlockSpec(memory_space=pltpu.VMEM)
    hbm = pl.BlockSpec(memory_space=pl.ANY)
    V = pltpu.VMEM
    own, others = pl.pallas_call(
        kernel,
        out_shape=[jax.ShapeDtypeStruct((3, 2048), F32)] * 2,
        in_specs=[hbm] * 12,
        out_specs=[vmem] * 2,
        scratch_shapes=[
            V((3, 2048), F32), V((3, 2048), F32), V((M, 128), F32), V((4, 1, 32), I32),
            V((4, 32), I32), V((4, 1, 512), I32), V((4, 512), I32), pltpu.SMEM((4, 32), I32),
            pltpu.SMEM((4, 32), I32),
            V((4, M, M), BF16), V((2, M, M), BF16), V((M, M), F32), V((512, 512), BF16),
            V((2, M, M), BF16),
            V((8, 2048), F32), V((128, 128), F32), V((128, 128), F32), V((384, 128), BF16), V((32, 8, 128), F32),
            V((6, 16, 128), F32), V((16, K, 128), F32), V((16, K, 128), F32), V((M, 128), F32),
            V((4, 4, 128), F32), V((3, 4, 128), F32), V((4, 8, 512), F32),
            V((NZ, 4, 128), BF16), V((NX, NZ, 4, 128), BF16), V((4, 16, 128), BF16),
            V((4, 16, 128), BF16), V((4, M), F32), V((3, 4, M), F32), V((8, 128), F32), V((128, 512), F32),
            V((NZ, NX, 8, 128), BF16), V((NZ, NX, 8, 128), BF16), V((NX, NZ, 8, 128), BF16),
            V((512, 512), F32), V((M, 128), F32), V((3, 16, 128), F32), V((128, 128), F32),
            V((3, 16, 128), F32), V((3, 16, 128), BF16), V((3, 3, 16, 128), BF16),
            pltpu.SemaphoreType.DMA((12,)), pltpu.SemaphoreType.DMA((13,)),
            pltpu.SemaphoreType.DMA((13,)),
        ],
        compiler_params=pltpu.CompilerParams(collective_id=0, has_side_effects=True),
    )(
        offsets, vel_cot, shell, leaf_dest[0].transpose(1, 2, 0), leaf_slot[0].T,
        coarse_dest[0].transpose(1, 2, 0), coarse_slot[0].T, near_box.T, near_dir.T, child_ops,
        m2l_ops, check_map,
    )
    return own + others


def solution(mesh):
    return jax.shard_map(
        local_part,
        mesh=mesh,
        in_specs=(
            P(None, "leaf"), P(None, "leaf"), P("lvl", None, None), P("lvl", None, None), P(),
            P("lvl", "leaf", None, None), P("lvl", "leaf", None), P("lvl", None, None, None),
            P("lvl", None, None), P("leaf", "lvl"), P("leaf", "lvl"),
        ),
        out_specs=P(None, "leaf"),
        check_vma=False,
    )
```

```python
import jax
import jax.numpy as jnp
import numpy as np
from jax import lax
from jax.experimental import pallas as pl
from jax.experimental.pallas import tpu as pltpu
from jax.sharding import PartitionSpec as P

SIDE = 6
EPS = 0.01
RADIUS = 0.525
M = 456
K = 152
NZ, NX, NL = 16, 8, 4
CH = 120
NEAREST = 4
F32, BF16, I32 = jnp.float32, jnp.bfloat16, jnp.int32
MESH = pl.DeviceIdType.MESH


def surface_points():
    levels = np.linspace(-1.0, 1.0, SIDE)
    lattice = np.stack(np.meshgrid(levels, levels, levels, indexing="ij"), 0).reshape(3, -1)
    on_shell = np.max(np.abs(lattice), 0) > 1.0 - 1e-09
    return (lattice[:, on_shell] * RADIUS).astype(np.float32)


def iota(shape, dim):
    return lax.broadcasted_iota(jnp.int32, shape, dim)


def dot(a, b, dims=((1,), (0,))):
    return lax.dot_general(a, b, (dims, ((), ())), preferred_element_type=F32)


def one_hot(hits):
    return jnp.where(hits, 1.0, 0.0).astype(BF16)


def kernel(
    off_h, vel_h, shell_h, leaf_dest_h, leaf_slot_h, coarse_dest_h, coarse_slot_h, near_box_h,
    near_dir_h, child_h, m2l_h, cm_h, own_ref, others_ref,
    off, vel, shell, leaf_dest, leaf_slot, coarse_dest, coarse_slot, near_box, near_dir,
    m2l, child, cm, cmt, down, x6, nat, tn, thirds, tab, xg, wst, qst, av, ppb, prs, ids, gz, pall, spb, spr,
    cpb, cpr, meta, tms, sb, rb, fin, wt, fl, nn, fo, frb, frs, frr,
    loc, ss, rs,
):
    me, lv = lax.axis_index("leaf"), lax.axis_index("lvl")
    zi, xi = me // NX, lax.rem(me, NX)

    def z_peer(k):
        return lax.rem(zi + k, NZ)

    def x_peer(k):
        return lax.rem(xi + k, NX)

    def y_peer(k):
        return lax.rem(lv + k, NL)

    barrier = pltpu.get_barrier_semaphore()

    def greet_z(k, c):
        pl.semaphore_signal(barrier, 1, device_id=(z_peer(k) * NX + xi, lv), device_id_type=MESH)
        return c

    def greet_x(k, c):
        pl.semaphore_signal(barrier, 1, device_id=(zi * NX + x_peer(k), lv), device_id_type=MESH)
        return c

    def greet_y(k, c):
        pl.semaphore_signal(barrier, 1, device_id=(me, y_peer(k)), device_id_type=MESH)
        return c

    loads = [
        pltpu.make_async_copy(src, dst, loc.at[n])
        for n, (src, dst) in enumerate(
            (
                (off_h, off), (vel_h, vel), (shell_h, shell), (leaf_dest_h, leaf_dest),
                (leaf_slot_h, leaf_slot), (coarse_dest_h, coarse_dest),
                (coarse_slot_h, coarse_slot), (near_box_h, near_box), (near_dir_h, near_dir),
                (child_h, child), (m2l_h, m2l), (cm_h, cm),
            )
        )
    ]
    for load in loads[0:3]:
        load.start()
    for k in (8, 7, 9, 6, 10, 5, 11, 4, 12, 3, 13, 2, 14, 1, 15):
        greet_z(k, 0)
    lax.fori_loop(1, NX, greet_x, 0)
    lax.fori_loop(1, NL, greet_y, 0)
    for n in (9, 3, 4, 5, 6, 10, 7, 8, 11):
        loads[n].start()

    def send(src, dst, phase, device):
        pltpu.make_async_remote_copy(
            src_ref=src, dst_ref=dst, send_sem=ss.at[phase], recv_sem=rs.at[phase],
            device_id=device, device_id_type=MESH,
        ).start()

    def arrived(ref, phase):
        pltpu.make_async_copy(ref, ref, rs.at[phase]).wait()

    def gone(ref, phase):
        pltpu.make_async_copy(ref, ref, ss.at[phase]).wait()

    groups = ((0, 8), (8, 4), (12, 4))

    def group_of(slot):
        return 3 if slot < 8 else 9 if slot < 12 else 10

    def forward(g):
        first, count = groups[g]
        arrived(rb.at[pl.ds(first, count - (g == 2))], group_of(first))
        for i in (4, 3, 5, 2, 6, 1, 7):
            src, dst = rb.at[pl.ds(first, count), x_peer(i)], fin.at[i - 1, pl.ds(first, count)]
            send(src, dst, 11 if g == 2 else 6, (zi * NX + x_peer(i), lv))

    for load in loads[0:3]:
        load.wait()
    x6[0:3] = off[...]
    x6[3:6] = vel[...]
    x6[6:8] = jnp.zeros((2, 2048), F32)
    low = iota((8, 128), 1) < 64
    for m in range(16):
        v = x6[:, m * 128 : (m + 1) * 128]
        nat[pl.ds(m, 8, stride=16), :] = v
        r = pltpu.roll(v, 64, 1)
        tab[2 * m] = jnp.where(low, v, r)
        tab[2 * m + 1] = jnp.where(low, r, v)
    tn[...] = nat[...].T
    lane16 = iota((16, 128), 1) // 16
    for c in range(3):
        whole = tn[...] if c == 0 else pltpu.roll(tn[...], 128 - 16 * c, 1)
        whole = jnp.where(iota((128, 128), 1) < 16, whole, 0.0)
        high = whole.astype(BF16).astype(F32)
        middle = (whole - high).astype(BF16).astype(F32)
        lowest = whole - high - middle
        split = high + pltpu.roll(middle, 16, 1) + pltpu.roll(lowest, 32, 1)
        thirds[c * 128 : (c + 1) * 128, :] = split.astype(BF16)
    for c in range(6):
        total = jnp.zeros((16, 128), F32)
        for b2 in range(2):
            for g in range(4):
                j, pos = b2 * 4 + g, g * 2 + b2
                piece = pltpu.roll(tn[16 * j : 16 * j + 16, :], (16 * (pos - c)) % 128, 1)
                total = jnp.where(lane16 == pos, piece, total)
        xg[c] = total

    def to_surface(kb, carry):
        row = pl.multiple_of(kb * 8, 8)
        s = [shell[pl.ds(c * K + row, 8), :] for c in range(3)]
        acc = [jnp.zeros((8, 128), F32) for _ in range(3)]
        for i in range(16):
            r = [s[c] - xg[c, i : i + 1, :] for c in range(3)]
            v = [xg[3 + c, i : i + 1, :] for c in range(3)]
            t = r[0] * r[0] + r[1] * r[1] + r[2] * r[2] + EPS
            inv = lax.rsqrt(t)
            w = inv * inv * inv
            q = w * (t + EPS)
            wd = w * (r[0] * v[0] + r[1] * v[1] + r[2] * v[2])
            for c in range(3):
                acc[c] = acc[c] + (q * v[c] + wd * r[c])
            wst[i, pl.ds(row, 8), :] = w
            qst[i, pl.ds(row, 8), :] = q
        for c in range(3):
            av[pl.ds(c * K + row, 8), :] = acc[c]
        return carry

    lax.fori_loop(0, K // 8, to_surface, 0)
    a = av[...]
    a = a + pltpu.roll(a, 64, 1)
    a = a + pltpu.roll(a, 32, 1)
    b_row, b_lane = iota((32, 128), 0), iota((32, 128), 1)
    pick = one_hot(b_lane == lax.rem(b_row, 2) * 16 + b_row // 2)
    summed = a.astype(BF16)
    local = dot(pick, summed, ((1,), (1,))).astype(BF16)

    for load in loads[3:7]:
        load.wait()
    for c in range(4):
        ids[lv, c : c + 1, :] = coarse_dest[c].astype(F32)
    ids[lv, 4:8, :] = coarse_slot[...].astype(F32)
    meta[...] = jnp.zeros((8, 128), F32)
    for c in range(4):
        meta[c : c + 1, 0:32] = leaf_dest[c].astype(F32)
    meta[4:8, 0:32] = leaf_slot[...].astype(F32)

    p_row, p_lane = iota((8, 128), 0), iota((8, 128), 1)
    loads[9].wait()
    part = jnp.zeros((8, M), F32)
    for o in range(2):
        rows = one_hot((p_lane == o * 16 + p_row * 4 + lv) & (p_row < 4))
        part = part + dot(dot(rows, summed, ((1,), (1,))).astype(BF16), child[o])
    ppb[3] = jnp.zeros((4, 128), F32)
    for k in range(3):
        ppb[k] = part[0:4, k * 128 : (k + 1) * 128]
    ppb[3, :, 0 : M - 384] = part[0:4, 384:M]
    pl.semaphore_wait(barrier, NZ + NX + NL - 3)
    for i in range(1, NL):
        send(ppb.at[y_peer(i)], prs.at[i - 1], 0, (me, y_peer(i)))

    loads[10].wait()
    tms[:, 384:512] = jnp.zeros((128, 128), F32)
    for c in range(4):
        tms[c * 32 : (c + 1) * 32, 0:M] = dot(local, m2l[c])
    lane32 = iota((1, 128), 1) // 32
    listed = []
    for first in (0, 4):
        line = meta[first : first + 1, :]
        for c in range(1, 4):
            line = jnp.where(lane32 == c, pltpu.roll(meta[first + c : first + c + 1, :], 32 * c, 1), line)
        listed.append(line)
    own = jnp.broadcast_to(listed[0], (128, 128))
    place = jnp.broadcast_to(listed[1], (128, 128)).T
    sub, lane = iota((128, 128), 0), iota((128, 128), 1)
    rank = jnp.sum(jnp.where((own.T == own) & (sub < lane), 1.0, 0.0), axis=0, keepdims=True)
    pos = (listed[0] * 2.0 + rank).astype(jnp.int32) * 4
    keys = jnp.concatenate([pos + j for j in range(4)], axis=1)
    flat = tms[...]
    pieces = []
    for j in range(4):
        piece = flat if j == 0 else pltpu.roll(flat, 512 - CH * j, 1)
        piece = jnp.where(lane < CH, piece[:, 0:128], jnp.where(lane == 127, place + 1.0, 0.0))
        pieces.append(piece.astype(BF16))
    pieces = jnp.concatenate(pieces, axis=0)
    for q in range(4):
        hits = one_hot(iota((256, 512), 0) + q * 256 == keys)
        sb[q * 4 : (q + 1) * 4] = dot(hits, pieces).reshape(4, 8, 8, 128).astype(BF16)
    rb[15] = sb[zi]

    def leaf_z(first, last):
        for slot in range(first, last):
            k = 1 + slot // 2 if slot % 2 == 0 else NZ - 1 - slot // 2
            send(sb.at[z_peer(k)], rb.at[slot], group_of(slot), (z_peer(k) * NX + xi, lv))

    leaf_z(0, NEAREST)

    arrived(prs, 0)
    mine = ppb[lv] + prs[0] + prs[1] + prs[2]
    gz[4] = mine.astype(BF16)
    for k in (8, 7, 9, 6, 10, 5, 11, 4, 12, 3, 13, 2, 14, 1, 15):
        slot = (4 - k) % NZ
        send(gz.at[4], gz.at[slot], 2 if slot < 9 else 12, (z_peer(k) * NX + xi, lv))
    leaf_z(NEAREST, 15)
    for i in range(1, NL):
        send(ids.at[lv], ids.at[lv], 1, (me, y_peer(i)))

    row8 = iota((8, 128), 0)
    loads[7].wait()
    loads[8].wait()

    def digits(code):
        by9, by3 = (code * 57) >> 9, (code * 43) >> 7
        return by9 - 1, by3 - 3 * by9 - 1, code - 3 * by3 - 1

    def near(m, carry):
        chosen = one_hot(lax.rem(iota((48, 128), 0), 16) == m)
        targets = dot(thirds[:, 0:48], chosen)
        columns = [[], [], []]
        for b2 in range(2):
            box = 2 * m + b2
            sources = []
            for pair in range(2):
                n1, n2 = 2 * pair, 2 * pair + 1
                d1, d2 = near_dir[n1, box], near_dir[n2, box]
                moved = jnp.where(low, tab[near_box[n1, box]], tab[near_box[n2, box]])
                parts = [digits(d) for d in (d1, d2)]
                shift = jnp.zeros((8, 128), F32)
                for c in range(3):
                    both = jnp.where(low, parts[0][c].astype(F32), parts[1][c].astype(F32))
                    shift = jnp.where(row8 == c, both, shift)
                moved = moved + shift
                sources.append([jnp.broadcast_to(moved[c : c + 1, :], (8, 128)) for c in range(6)])
            for tv in range(8):
                at = b2 * 64 + tv * 8
                x = [targets[c * 128 + at : c * 128 + at + 8, :] for c in range(3)]
                acc = [jnp.zeros((8, 128), F32) for _ in range(3)]
                for src in sources:
                    r = [x[c] - src[c] for c in range(3)]
                    t = r[0] * r[0] + r[1] * r[1] + r[2] * r[2] + EPS
                    inv = lax.rsqrt(t)
                    w = inv * inv * inv
                    q = w * (t + EPS)
                    wd = w * (r[0] * src[3] + r[1] * src[4] + r[2] * src[5])
                    for c in range(3):
                        acc[c] = acc[c] + (q * src[3 + c] + wd * r[c])
                for c in range(3):
                    columns[c].append(acc[c])
        for c in range(3):
            total = jnp.concatenate(columns[c], axis=0)
            high = total.astype(BF16)
            rest = (total - high.astype(F32)).astype(BF16)
            both = jnp.concatenate([high, rest], axis=1)
            nn[c, pl.ds(m, 1), :] = dot(jnp.ones((8, 256), BF16), both, ((1,), (1,)))[0:1, :]
        return carry

    lax.fori_loop(0, 16, near, 0, unroll=2)

    loads[11].wait()
    wt[...] = jnp.zeros((512, 512), F32)
    wt[0:M, 0:M] = cm[...]
    cmt[...] = wt[...].T.astype(BF16)

    for first, count, phase in ((0, 9, 2), (9, 7, 12)):
        arrived(gz.at[pl.ds(first, min(count, 8))], phase)
        for i in (4, 3, 5, 2, 6, 1, 7):
            part = gz.at[pl.ds(first, count)]
            send(part, pall.at[xi, pl.ds(first, count)], 4, (zi * NX + x_peer(i), lv))
    pall[xi] = gz[...]
    for o in range(2):
        down[o] = dot(cmt[0:M, 0:M], child[o]).astype(BF16)
    arrived(ids.at[pl.ds(0, NL - 1)], 1)
    col = iota((512, 512), 1)
    plane = lax.rem(zi + lax.rem(col // 4, NZ) + 12, NZ)
    gathered = (plane * NX + col // 64) * 4 + lax.rem(col, 4)
    order = one_hot(iota((512, 512), 0) == gathered)
    listed = dot(ids[...].reshape(32, 512).astype(BF16), order)
    parents = iota((8, 512), 0)
    wanted = (me * 4 + lax.rem(parents, 4)).astype(F32)
    selects = []
    for l in range(NL):
        for c in (0, 2):
            first, second = (
                listed[8 * l + n : 8 * l + n + 1, :] * 4.0 + listed[8 * l + 4 + n : 8 * l + 5 + n, :]
                for n in (c, c + 1)
            )
            named = jnp.where(parents < 4, first, second)
            selects.append(jnp.where(named == wanted, 1.0, 0.0))
    select = jnp.concatenate(selects, axis=0).astype(BF16)
    forward(0)
    arrived(pall.at[pl.ds(0, NX - 1)], 4)
    coarse = [
        jnp.concatenate([pall[x, 2 * z].astype(F32), pall[x, 2 * z + 1].astype(F32)], axis=0)
        for x in range(NX)
        for z in range(NZ // 2)
    ]
    coarse = jnp.concatenate(coarse, axis=0).astype(BF16)
    spb[...] = dot(select, coarse).reshape(4, 16, 128).astype(BF16)
    for i in range(1, NL):
        send(spb.at[y_peer(i)], spr.at[lv], 5, (me, y_peer(i)))
    spr[lv] = spb[lv]

    forward(1)

    arrived(spr.at[pl.ds(0, NL - 1)], 5)
    rows = jnp.concatenate([spr[k].astype(F32) for k in range(4)], axis=1)[:, 0:M]
    part = jnp.zeros((16, M), F32)
    for c in range(4):
        part = part + dot(jnp.where(iota((16, M), 0) // 4 == c, rows, 0.0).astype(BF16), m2l[c])
    part = part[0:8] + part[8:16]
    cpb[...] = 0.5 * (part[0:4] + part[4:8])
    for i in range(1, NL):
        send(cpb, cpr.at[i - 1], 7, (me, y_peer(i)))
    forward(2)
    def box_of(lanes):
        beta = lax.rem(lanes, 32)
        return 2 * lax.rem(beta, 16) + beta // 16

    def landed(first, count, phase):
        fin[7, first : first + count] = rb[first : first + count, xi]
        arrived(fin.at[pl.ds(0, NX - 1), pl.ds(first, count)], phase)
        size = NX * count * 8
        got = fin[:, first : first + count].astype(F32).reshape(size, 128)
        ident = got[:, 127:128]
        quarter = lax.rem(iota((size, 1), 0), 4).astype(F32)
        key = jnp.where(ident > 0.5, ident - 1.0 + 32.0 * quarter, -1.0)
        landing = one_hot(key.astype(jnp.int32) == iota((size, 128), 1))
        return dot(got.astype(BF16), landing, ((0,), (0,)))

    leaf_sum = landed(0, 12, 6)
    arrived(cpr, 7)
    parent = jnp.concatenate([cpb[...] + cpr[0] + cpr[1] + cpr[2], jnp.zeros((4, M), F32)], axis=0)
    p_box = box_of(iota((8, 128), 1))
    lowered = jnp.zeros((M, 128), F32)
    for o in range(2):
        spread = one_hot((p_box // 8 == row8) & (lax.rem(p_box, 8) == lv * 2 + o))
        octant = dot(parent.astype(BF16), spread, ((0,), (0,))).astype(BF16)
        lowered = lowered + dot(down[o], octant)
    leaf_sum = (leaf_sum + landed(12, 4, 11)).astype(BF16)
    e_box = box_of(lane)
    totals = [dot(leaf_sum[0:CH, :], one_hot(sub == 32 * j + e_box)) for j in range(4)]
    total = jnp.concatenate(totals, axis=0)[0:M, :].astype(BF16)
    fl[...] = dot(cmt[0:M, 0:M], total) + lowered

    def from_surface(i, carry):
        x = [jnp.broadcast_to(xg[c, pl.ds(i, 1), :], (8, 128)) for c in range(3)]
        acc = [jnp.zeros((8, 128), F32) for _ in range(3)]
        for kb in range(K // 8):
            at = kb * 8
            f = [fl[c * K + at : c * K + at + 8, :] for c in range(3)]
            r = [x[c] - shell[c * K + at : c * K + at + 8, :] for c in range(3)]
            q = qst[i, at : at + 8, :]
            wd = wst[i, at : at + 8, :] * (r[0] * f[0] + r[1] * f[1] + r[2] * f[2])
            for c in range(3):
                acc[c] = acc[c] + (q * f[c] + wd * r[c])
        for c in range(3):
            fo[pl.ds(c * 16 + i, 1), :] = jnp.sum(acc[c], axis=0, keepdims=True)
        return carry

    fo[48:128] = jnp.zeros((80, 128), F32)
    lax.fori_loop(0, 16, from_surface, 0, unroll=4)
    back = fo[...].T
    for c in range(3):
        total = jnp.zeros((16, 128), F32)
        for b2 in range(2):
            for g in range(4):
                at = g * 32 + b2 * 16
                pos = b2 * 4 + g
                piece = pltpu.roll(back[at : at + 16, :], (16 * (pos - c)) % 128, 1)
                total = jnp.where(lane16 == pos, piece, total)
        frb[c] = total + nn[c]
    frs[...] = frb[...].astype(BF16)
    for i in range(1, NL):
        send(frs, frr.at[i - 1], 8, (me, y_peer(i)))

    def spread_out(ref, forces):
        for c in range(3):
            for m in range(16):
                ref[c : c + 1, m * 128 : (m + 1) * 128] = forces[c, m : m + 1, :]

    spread_out(own_ref, frb[...])
    arrived(frr, 8)
    spread_out(others_ref, frr[0].astype(F32) + frr[1].astype(F32) + frr[2].astype(F32))

    gone(ppb.at[pl.ds(0, NL - 1)], 0)
    gone(ids.at[pl.ds(0, NL - 1)], 1)
    gone(gz.at[pl.ds(0, 8)], 2)
    gone(gz.at[pl.ds(0, 7)], 12)
    gone(rb.at[pl.ds(0, 8)], 3)
    gone(rb.at[pl.ds(0, 4)], 9)
    gone(rb.at[pl.ds(0, 3)], 10)
    gone(pall.at[pl.ds(0, NX - 1)], 4)
    gone(spb.at[pl.ds(0, NL - 1)], 5)
    gone(fin.at[pl.ds(0, NX - 1), pl.ds(0, 12)], 6)
    gone(fin.at[pl.ds(0, NX - 1), pl.ds(0, 4)], 11)
    gone(cpr, 7)
    gone(frr, 8)


def local_part(
    offsets, vel_cot, m2l_ops, child_ops, check_map, leaf_dest, leaf_slot, coarse_dest,
    coarse_slot, near_box, near_dir,
):
    shell = jnp.asarray(np.repeat(surface_points().reshape(M, 1), 128, axis=1))
    vmem = pl.BlockSpec(memory_space=pltpu.VMEM)
    hbm = pl.BlockSpec(memory_space=pl.ANY)
    V = pltpu.VMEM
    own, others = pl.pallas_call(
        kernel,
        out_shape=[jax.ShapeDtypeStruct((3, 2048), F32)] * 2,
        in_specs=[hbm] * 12,
        out_specs=[vmem] * 2,
        scratch_shapes=[
            V((3, 2048), F32), V((3, 2048), F32), V((M, 128), F32), V((4, 1, 32), I32),
            V((4, 32), I32), V((4, 1, 512), I32), V((4, 512), I32), pltpu.SMEM((4, 32), I32),
            pltpu.SMEM((4, 32), I32),
            V((4, M, M), BF16), V((2, M, M), BF16), V((M, M), F32), V((512, 512), BF16),
            V((2, M, M), BF16),
            V((8, 2048), F32), V((128, 128), F32), V((128, 128), F32), V((384, 128), BF16), V((32, 8, 128), F32),
            V((6, 16, 128), F32), V((16, K, 128), F32), V((16, K, 128), F32), V((M, 128), F32),
            V((4, 4, 128), F32), V((3, 4, 128), F32), V((4, 8, 512), F32),
            V((NZ, 4, 128), BF16), V((NX, NZ, 4, 128), BF16), V((4, 16, 128), BF16),
            V((4, 16, 128), BF16), V((4, M), F32), V((3, 4, M), F32), V((8, 128), F32), V((128, 512), F32),
            V((NZ, NX, 8, 128), BF16), V((NZ, NX, 8, 128), BF16), V((NX, NZ, 8, 128), BF16),
            V((512, 512), F32), V((M, 128), F32), V((3, 16, 128), F32), V((128, 128), F32),
            V((3, 16, 128), F32), V((3, 16, 128), BF16), V((3, 3, 16, 128), BF16),
            pltpu.SemaphoreType.DMA((12,)), pltpu.SemaphoreType.DMA((13,)),
            pltpu.SemaphoreType.DMA((13,)),
        ],
        compiler_params=pltpu.CompilerParams(collective_id=0, has_side_effects=True),
    )(
        offsets, vel_cot, shell, leaf_dest[0].transpose(1, 2, 0), leaf_slot[0].T,
        coarse_dest[0].transpose(1, 2, 0), coarse_slot[0].T, near_box.T, near_dir.T, child_ops,
        m2l_ops, check_map,
    )
    return own + others


def solution(mesh):
    return jax.shard_map(
        local_part,
        mesh=mesh,
        in_specs=(
            P(None, "leaf"), P(None, "leaf"), P("lvl", None, None), P("lvl", None, None), P(),
            P("lvl", "leaf", None, None), P("lvl", "leaf", None), P("lvl", None, None, None),
            P("lvl", None, None), P("leaf", "lvl"), P("leaf", "lvl"),
        ),
        out_specs=P(None, "leaf"),
        check_vma=False,
    )
```
